128 devices in a mesh: replica: 2 (over core), fsdp: 16 (over y, x), tensor: 4 (over z).
Axes of the slice: x: 4, y: 4, z: 4, core: 2. Of those that a mesh axis runs over, the one named last changes fastest.
Arguments:
- grads: bfloat16 [2, 2, 4096, 14336], P('replica', None, 'fsdp', 'tensor'), may hold values from -6 to 6
- momentum: bfloat16 [2, 4096, 14336], P(None, 'fsdp', 'tensor'), may hold values from -50 to 50, as said below
- basis: bfloat16 [2, 14336, 512], P(None, 'tensor'), may hold values from -0.046875 to 0.046875
Outputs:
- momentum_new: bfloat16 [2, 4096, 14336], P(None, 'fsdp', 'tensor')
- update: bfloat16 [2, 4096, 14336], P(None, 'fsdp', 'tensor')
- basis_new: bfloat16 [2, 14336, 512], P(None, 'tensor')
The draws below stay inside these ranges and needn't reach their ends.
Inputs may be any that keep to these rules, and one draw needn't show every extreme that they name: `momentum`: entries are finite.
All inputs are finite; a program needn't handle non-finite values.
Results may differ from the reference program's by a relative error of at most 0.028.
Values may be sent and summed in bfloat16 or wider, within the bound.
A program may use at most 128 MiB of HBM per device.

```python
import math
import jax
import jax.numpy as jnp
from jax import lax

FEATURES = 4096
UNITS = 14336
RANK = 512
WEIGHTS = 2
REPLICAS = 2


def draw_momentum(key, part):
    first, second, third = jax.random.split(key, 3)
    shape = (WEIGHTS, FEATURES, UNITS)
    base = jnp.clip(jax.random.normal(first, shape, jnp.float32), -5.0, 5.0)
    top = math.log(10.0)
    row_scale = jnp.exp(jax.random.uniform(second, (WEIGHTS, FEATURES, 1), jnp.float32, 0.0, top) - 0.5 * top)
    col_scale = jnp.exp(jax.random.uniform(third, (WEIGHTS, 1, UNITS), jnp.float32, 0.0, top) - 0.5 * top)
    return (base * row_scale * col_scale).astype(jnp.bfloat16)


def levels(own_key, shape, cuts, least, top_value):
    gain, own = 1.0, jax.random.fold_in(own_key, 6)
    for position, parts in cuts:
        steps = jnp.exp(jax.random.uniform(jax.random.fold_in(own, position), (parts,), jnp.float32, least / len(cuts), top_value / len(cuts)))
        gain = gain * jnp.repeat(steps, shape[position] // parts).reshape([-1 if axis == position else 1 for axis in range(len(shape))])
    return gain


def scatter_about(key, dims, scale, limit, cuts=(), held_as=jnp.bfloat16):
    factor_of = levels(key, dims, cuts, -0.22, 0.18) if cuts else 1.0
    drawn = jax.random.normal(key, dims, jnp.float32) * scale * factor_of
    return jnp.minimum(jnp.maximum(drawn, -limit), limit).astype(held_as)


def setup_inputs(seed: int = 0) -> dict:
    key_list = jax.random.split(jax.random.key(seed), 4)
    return {
        "grads": scatter_about(key_list[0], (REPLICAS, WEIGHTS, FEATURES, UNITS), 1.0, 6.0, ((0, 2), (2, 16), (3, 4))),
        "momentum": draw_momentum(jax.random.fold_in(key_list[3], 71), 0),
        "basis": scatter_about(key_list[2], (WEIGHTS, UNITS, RANK), UNITS ** -0.5, 0.046875, ((1, 4),)),
    }


momentum_decay = 0.95

def one_weight(grad_stack, moment, right):
    total_grad = lax.optimization_barrier(jnp.sum(grad_stack.astype(jnp.float32), axis=0))
    blended = (moment.astype(jnp.float32) + total_grad).astype(jnp.bfloat16)
    projected = jnp.dot(blended.astype(jnp.float32), right.astype(jnp.float32), preferred_element_type=jnp.float32)
    gram_matrix = jnp.dot(projected.T.astype(jnp.float32), projected.astype(jnp.float32), preferred_element_type=jnp.float32, precision=lax.Precision.HIGHEST)
    factor = jnp.linalg.cholesky(gram_matrix)
    left_basis = jax.scipy.linalg.solve_triangular(factor, projected.T, lower=True).T.astype(jnp.bfloat16)
    back = jnp.dot(blended.T.astype(jnp.float32), left_basis.astype(jnp.float32), preferred_element_type=jnp.float32)
    col_norm = jnp.sqrt(lax.optimization_barrier(jnp.sum(back * back, axis=0))) + 1e-06
    back_b = back.astype(jnp.bfloat16)
    basis_new = (back_b.astype(jnp.float32) / col_norm[None, :]).astype(jnp.bfloat16)
    feedback = jnp.dot(left_basis.astype(jnp.float32), back_b.T.astype(jnp.float32), preferred_element_type=jnp.float32)
    momentum_new = (blended.astype(jnp.float32) - (1.0 - momentum_decay) * feedback).astype(jnp.bfloat16)
    scale = math.sqrt(FEATURES * UNITS / RANK)
    update = (scale * jnp.dot(left_basis.astype(jnp.float32), basis_new.T.astype(jnp.float32), preferred_element_type=jnp.float32)).astype(jnp.bfloat16)
    return (momentum_new, update, basis_new)

def reference(grads, momentum, basis):
    moments, updates, bases = ([], [], [])
    for which in range(WEIGHTS):
        result = one_weight(grads[:, which], momentum[which], basis[which])
        moments.append(result[0])
        updates.append(result[1])
        bases.append(result[2])
    return (jnp.stack(moments), jnp.stack(updates), jnp.stack(bases))
```

```python
import functools
import math

import jax
import jax.numpy as jnp
from jax import lax
from jax.experimental import pallas as pl
from jax.experimental.pallas import tpu as pltpu
from jax.sharding import Mesh
from jax.sharding import PartitionSpec as P

FEATURES = 4096
UNITS = 14336
RANK = 512
FSDP = ("fsdp_0", "fsdp_1")
MESH = pl.DeviceIdType.MESH
BF16 = jnp.bfloat16
F32 = jnp.float32
ROWS = FEATURES // 16
COLS = UNITS // 4
PIECE = COLS // 16
SLICE = ROWS // 4
STEP = 512
PANEL = 16
BLOCK = 128

momentum_decay = 0.95


def coords():
    return tuple(lax.axis_index(a) for a in ("replica", "fsdp_0", "fsdp_1", "tensor"))


def shifted(i, k):
    return lax.rem(i + k, 4)


class Ring:
    def __init__(self, axis, at, send, recv):
        self.axis, self.at, self.send, self.recv = axis, at, send, recv
        me = lax.axis_index(axis)
        self.me, self.right, self.left, self.far = me, shifted(me, 1), shifted(me, 3), shifted(me, 2)

    def copy(self, k, who, half, to):
        ref = self.at(who, half)
        return pltpu.make_async_remote_copy(
            src_ref=ref,
            dst_ref=ref,
            send_sem=self.send.at[k],
            recv_sem=self.recv.at[k],
            device_id={self.axis: to},
            device_id_type=MESH,
        )

    def start(self):
        self.copy(0, self.me, None, self.right).start()
        self.copy(1, self.me, None, self.left).start()

    def middle(self):
        self.copy(0, self.left, None, self.right).wait_recv()
        self.copy(2, self.left, 0, self.right).start()
        self.copy(1, self.right, None, self.left).wait_recv()
        self.copy(3, self.right, 1, self.left).start()

    def end(self):
        self.copy(2, self.far, 0, self.right).wait_recv()
        self.copy(3, self.far, 1, self.left).wait_recv()

    def drain(self):
        self.copy(0, self.me, None, self.right).wait_send()
        self.copy(1, self.me, None, self.left).wait_send()
        self.copy(2, self.left, 0, self.right).wait_send()
        self.copy(3, self.right, 1, self.left).wait_send()


def rows_of(start, size, half):
    if half is None:
        return pl.ds(start, size)
    return pl.ds(start + half * (size // 2), size // 2)


def projected_rings(full, y, x, z, send, recv):
    parts = ((0, 32, 0, 384), (32, 32, 0, 384), (0, 64, 384, 128))

    def cut(part, half):
        r0, nr, c0, nc = parts[part]
        return rows_of(r0, nr, half), pl.ds(c0, nc)

    every = slice(None)
    plans = (
        (0, 0, "tensor", lambda i: (y, x, i)),
        (0, 1, "fsdp_0", lambda i: (i, x, every)),
        (0, 2, "fsdp_1", lambda i: (every, i, every)),
        (1, 0, "fsdp_1", lambda i: (y, i, z)),
        (1, 1, "tensor", lambda i: (y, every, i)),
        (1, 2, "fsdp_0", lambda i: (i, every, every)),
        (2, 0, "fsdp_0", lambda i: (i, x, z)),
        (2, 1, "fsdp_1", lambda i: (every, i, z)),
        (2, 2, "tensor", lambda i: (every, every, i)),
    )
    phases = ([], [], [])
    for part, phase, axis, where in plans:
        def at(i, half, part=part, where=where):
            return full.at[(*where(i), *cut(part, half))]

        phases[phase].append(Ring(axis, at, send.at[part, phase], recv.at[part, phase]))
    return phases


def blend_kernel(
    grads, momentum, basis, full, turned, blended,
    m_v, g_v, gp_v, b_v, acc, flipped, out_z, in_z,
    load, gs, gr, zs, zr, ags, agr, ts, tr, ps, pr,
):
    r, y, x, z = coords()
    other = 1 - r
    steps = COLS // STEP

    def grad_copy(c, cols):
        return pltpu.make_async_remote_copy(
            src_ref=grads.at[0, other, :, cols],
            dst_ref=gp_v.at[:, cols],
            send_sem=gs.at[c],
            recv_sem=gr.at[c],
            device_id={"replica": other},
            device_id_type=MESH,
        )

    def loads(c, cols):
        return (
            pltpu.make_async_copy(grads.at[0, r, :, cols], g_v.at[:, cols], load.at[0, c]),
            pltpu.make_async_copy(momentum.at[r, :, cols], m_v.at[:, cols], load.at[1, c]),
            pltpu.make_async_copy(basis.at[r, cols, :], b_v.at[cols, :], load.at[2, c]),
        )

    for c in range(steps):
        cols = pl.ds(c * STEP, STEP)
        grad_copy(c, cols).start()
        for copy in loads(c, cols):
            copy.start()
    acc[...] = jnp.zeros_like(acc)

    def blend(c, carry):
        cols = pl.ds(pl.multiple_of(c * STEP, STEP), STEP)
        for copy in loads(c, cols):
            copy.wait()
        grad_copy(c, cols).wait()
        total = g_v[:, cols].astype(F32) + gp_v[:, cols].astype(F32)
        value = (m_v[:, cols].astype(F32) + total).astype(BF16)
        blended[r, :, cols] = value
        flipped[cols, :] = value.T
        acc[...] += jnp.dot(value, b_v[cols, :], preferred_element_type=F32)
        return carry

    lax.fori_loop(0, steps, blend, 0)

    def z_copy(k):
        return pltpu.make_async_remote_copy(
            src_ref=out_z.at[k - 1],
            dst_ref=in_z.at[k - 1],
            send_sem=zs.at[k - 1],
            recv_sem=zr.at[k - 1],
            device_id={"tensor": shifted(z, k)},
            device_id_type=MESH,
        )

    for k in (2, 1, 3):
        rows = pl.ds(pl.multiple_of(shifted(z, k) * SLICE, SLICE), SLICE)
        out_z[k - 1] = acc[rows, :].astype(BF16)
        z_copy(k).start()
    total = acc[pl.ds(pl.multiple_of(z * SLICE, SLICE), SLICE), :]
    for k in (1, 3, 2):
        z_copy(k).wait()
        total = total + in_z[k - 1].astype(F32)
    full[y, x, z] = total.astype(BF16)

    phases = projected_rings(full, y, x, z, ags, agr)
    for phase in phases:
        for ring in phase:
            ring.start()
        for ring in phase:
            ring.middle()
        if phase is not phases[-1]:
            for ring in phase:
                ring.end()

    def turn_copy(k):
        ty, tx = shifted(y, k // 4), shifted(x, k % 4)
        start = pl.multiple_of((ty * 4 + tx) * PIECE, PIECE)
        return pltpu.make_async_remote_copy(
            src_ref=flipped.at[pl.ds(start, PIECE), :],
            dst_ref=turned.at[y, x],
            send_sem=ts.at[k],
            recv_sem=tr.at[k],
            device_id={"fsdp_0": ty, "fsdp_1": tx},
            device_id_type=MESH,
        )

    def turn_arrival(k):
        sy, sx = shifted(y, 4 - k // 4), shifted(x, 4 - k % 4)
        return pltpu.make_async_remote_copy(
            src_ref=turned.at[sy, sx],
            dst_ref=turned.at[sy, sx],
            send_sem=ts.at[k],
            recv_sem=tr.at[k],
            device_id={"fsdp_0": sy, "fsdp_1": sx},
            device_id_type=MESH,
        )

    for k in range(1, 16):
        turn_copy(k).start()
    share = pltpu.make_async_remote_copy(
        src_ref=blended.at[r],
        dst_ref=blended.at[r],
        send_sem=ps.at[0],
        recv_sem=pr.at[0],
        device_id={"replica": other},
        device_id_type=MESH,
    )
    share.start()
    turned[y, x] = flipped[pl.ds(pl.multiple_of((y * 4 + x) * PIECE, PIECE), PIECE), :]
    for ring in phases[-1]:
        ring.end()
    for phase in phases:
        for ring in phase:
            ring.drain()
    for k in range(1, 16):
        turn_copy(k).wait_send()
        turn_arrival(k).wait_recv()
    share.wait_send()
    pltpu.make_async_remote_copy(
        src_ref=blended.at[other],
        dst_ref=blended.at[other],
        send_sem=ps.at[0],
        recv_sem=pr.at[0],
        device_id={"replica": other},
        device_id_type=MESH,
    ).wait_recv()


def halves(value):
    high = value.astype(BF16)
    return high, (value - high.astype(F32)).astype(BF16)


def contract_rows(a, b):
    ah, al = halves(a)
    bh, bl = halves(b)
    return lax.dot_general(
        jnp.concatenate([ah, ah, al], axis=0),
        jnp.concatenate([bh, bl, bh], axis=0),
        (((0,), (0,)), ((), ())),
        preferred_element_type=F32,
    )


def product(a, b):
    ah, al = halves(a)
    bh, bl = halves(b)
    return jnp.dot(
        jnp.concatenate([ah, ah, al], axis=1),
        jnp.concatenate([bh, bl, bh], axis=0),
        preferred_element_type=F32,
    )


def eliminate(work, inverse):
    row = lax.broadcasted_iota(jnp.int32, (PANEL, BLOCK), 0)
    lane = lax.broadcasted_iota(jnp.int32, (BLOCK, BLOCK), 1)

    def panel(p, carry):
        left, right = work[0:PANEL, 0:BLOCK], work[0:PANEL, BLOCK:]
        columns = [jnp.broadcast_to(left[:, k : k + 1], (PANEL, BLOCK)) for k in range(PANEL)]
        inverses = jnp.ones((PANEL, BLOCK), F32)
        for j in range(PANEL):
            inv = 1.0 / columns[j][j : j + 1, :]
            times = jnp.where(row > j, columns[j] * inv, 0.0)
            for k in range(j + 1, PANEL):
                columns[k] = columns[k] - times * columns[k][j : j + 1, :]
            left = left - times * left[j : j + 1, :]
            right = right - times * right[j : j + 1, :]
            inverses = jnp.where(row == j, inv, inverses)
        scale = jnp.sqrt(inverses)
        left, right = left * scale, right * scale
        inverse[pl.ds(pl.multiple_of(p * PANEL, PANEL), PANEL), :] = right
        change = contract_rows(left, jnp.concatenate([left, right], axis=1))
        rest = work[:, 0:BLOCK] - change[:, 0:BLOCK]
        rest = jnp.where(lane < BLOCK - PANEL, pltpu.roll(rest, BLOCK - PANEL, 1), 0.0)
        work[0 : BLOCK - PANEL, 0:BLOCK] = rest[PANEL:, :]
        extra = work[:, BLOCK:] - change[:, BLOCK:]
        work[0 : BLOCK - PANEL, BLOCK:] = extra[PANEL:, :]
        work[BLOCK - PANEL :, :] = jnp.zeros((PANEL, 2 * BLOCK), F32)
        return carry

    lax.fori_loop(0, BLOCK // PANEL, panel, 0)


def factor_inverse(gram, low, work, inverse):
    low[...] = jnp.zeros_like(low)
    count = RANK // BLOCK
    square = (BLOCK, BLOCK)
    eye = jnp.where(
        lax.broadcasted_iota(jnp.int32, square, 0) == lax.broadcasted_iota(jnp.int32, square, 1), 1.0, 0.0
    )
    for k in range(count):
        here, after = slice(k * BLOCK, (k + 1) * BLOCK), slice((k + 1) * BLOCK, RANK)
        work[:, 0:BLOCK] = gram[here, here]
        work[:, BLOCK:] = eye
        eliminate(work, inverse)
        block = inverse[...]
        if k:
            low[here, 0 : k * BLOCK] = product(block, low[here, 0 : k * BLOCK])
        low[here, here] = block
        if k < count - 1:
            upper = product(block, gram[here, after])
            gram[after, after] = gram[after, after] - contract_rows(upper, upper)
            done = slice(0, (k + 1) * BLOCK)
            low[after, done] = low[after, done] - contract_rows(upper, low[here, done])


def basis_kernel(full, turned, own, back, squares, gram, low, work, inverse, total):
    _, y, x, _ = coords()
    gram[...] = jnp.zeros_like(gram)

    def add_gram(b, carry):
        rows = full[b]
        gram[...] += lax.dot_general(rows, rows, (((0,), (0,)), ((), ())), preferred_element_type=F32)
        return carry

    lax.fori_loop(0, 16, add_gram, 0)
    factor_inverse(gram, low, work, inverse)
    high, rest = halves(low[...])
    total[...] = jnp.zeros_like(total)
    dims = (((1,), (1,)), ((), ()))

    def left_rows(b):
        rows = full[b]
        value = lax.dot_general(rows, high, dims, preferred_element_type=F32)
        value += lax.dot_general(rows, rest, dims, preferred_element_type=F32)
        return value.astype(BF16)

    def add_back(b, carry):
        total[...] += jnp.dot(turned[b], left_rows(b), preferred_element_type=F32)
        return carry

    lax.fori_loop(0, 16, add_back, 0)
    own[...] = left_rows(y * 4 + x)
    value = total[...]
    back[...] = value.astype(BF16)
    squares[...] = jnp.sum((value * value).reshape(PIECE // 8, 8, RANK), axis=0)


def gather_kernel(back, squares, own, full, norms, left, sums, s_ag, r_ag, s_n, r_n, s_p, r_p, local):
    r, y, x, z = coords()
    other = 1 - r
    place = (
        pltpu.make_async_copy(back, full.at[r, y, x], local.at[0]),
        pltpu.make_async_copy(own, left.at[r], local.at[1]),
    )
    for copy in place:
        copy.start()

    def sum_copy(phase, axis, k, me):
        return pltpu.make_async_remote_copy(
            src_ref=sums.at[phase, me],
            dst_ref=sums.at[phase, me],
            send_sem=s_n.at[phase, k - 1],
            recv_sem=r_n.at[phase, k - 1],
            device_id={axis: shifted(me, k)},
            device_id_type=MESH,
        )

    def sum_arrival(phase, axis, k, me):
        source = shifted(me, 4 - k)
        return pltpu.make_async_remote_copy(
            src_ref=sums.at[phase, source],
            dst_ref=sums.at[phase, source],
            send_sem=s_n.at[phase, k - 1],
            recv_sem=r_n.at[phase, k - 1],
            device_id={axis: source},
            device_id_type=MESH,
        )

    def send_sums(phase, axis, me, value):
        sums[phase, me] = value
        for k in (2, 1, 3):
            sum_copy(phase, axis, k, me).start()

    def take_sums(phase, axis, me):
        for k in (1, 3, 2):
            sum_arrival(phase, axis, k, me).wait_recv()
        return (sums[phase, 0] + sums[phase, 1]) + (sums[phase, 2] + sums[phase, 3])

    send_sums(0, "tensor", z, squares[...])
    for copy in place:
        copy.wait()

    halfcols = (pl.ds(0, RANK // 2), pl.ds(RANK // 2, RANK // 2))
    every = slice(None)

    def ring(part, phase, axis, where):
        def at(i, half):
            return full.at[(r, *where(i), rows_of(0, PIECE, half), halfcols[part])]

        return Ring(axis, at, s_ag.at[part, phase], r_ag.at[part, phase])

    first = (ring(0, 0, "fsdp_0", lambda i: (i, x)), ring(1, 0, "fsdp_1", lambda i: (y, i)))
    second = (ring(0, 1, "fsdp_1", lambda i: (every, i)), ring(1, 1, "fsdp_0", lambda i: (i, every)))

    def pass_on(k, src):
        return pltpu.make_async_remote_copy(
            src_ref=src,
            dst_ref=src,
            send_sem=s_p.at[k],
            recv_sem=r_p.at[k],
            device_id={"replica": other},
            device_id_type=MESH,
        )

    def group(weight, part, far):
        if part == 0:
            return full.at[weight, :, shifted(x, far), :, halfcols[part]]
        return full.at[weight, shifted(y, far), :, :, halfcols[part]]

    def partner(weight):
        jobs = [(part, far, pass_on(4 * part + far, group(weight, part, far))) for part in (0, 1) for far in range(4)]
        return {(part, far): job for part, far, job in jobs}

    mine, theirs = partner(r), partner(other)
    for g in first:
        g.start()
    pass_on(8, left.at[r]).start()
    for g in first:
        g.middle()
    value = take_sums(0, "tensor", z)
    send_sums(1, "fsdp_1", x, value)
    for g in first:
        g.end()
    for part, g in enumerate(second):
        g.start()
        mine[part, 0].start()
    value = take_sums(1, "fsdp_1", x)
    send_sums(2, "fsdp_0", y, value)
    value = take_sums(2, "fsdp_0", y)
    norms[r] = value
    pass_on(9, norms.at[r]).start()
    for part, g in enumerate(second):
        g.middle()
        mine[part, 1].start()
        mine[part, 3].start()
    for part, g in enumerate(second):
        g.end()
        mine[part, 2].start()
    for g in first + second:
        g.drain()
    for phase, axis, me in ((0, "tensor", z), (1, "fsdp_1", x), (2, "fsdp_0", y)):
        for k in (1, 2, 3):
            sum_copy(phase, axis, k, me).wait_send()
    pass_on(8, left.at[r]).wait_send()
    pass_on(9, norms.at[r]).wait_send()
    pass_on(8, left.at[other]).wait_recv()
    pass_on(9, norms.at[other]).wait_recv()
    for key in mine:
        mine[key].wait_send()
        theirs[key].wait_recv()


def output_kernel(left, back, blended, norms, momentum_new, update, basis_new):
    squares = jnp.sum(norms[0], axis=0, keepdims=True)
    inverse = 1.0 / (jnp.sqrt(squares) + 1e-06)
    rows = back[0]
    normed = (rows.astype(F32) * inverse).astype(BF16)
    basis_new[0] = normed
    dims = (((1,), (1,)), ((), ()))
    feedback = lax.dot_general(left[0], rows, dims, preferred_element_type=F32)
    momentum_new[0] = (blended[0].astype(F32) - (1.0 - momentum_decay) * feedback).astype(BF16)
    scale = math.sqrt(FEATURES * UNITS / RANK)
    update[0] = (scale * lax.dot_general(left[0], normed, dims, preferred_element_type=F32)).astype(BF16)


def shape(dims, dtype=BF16):
    return jax.ShapeDtypeStruct(dims, dtype)


VM = pl.BlockSpec(memory_space=pltpu.VMEM)
ANY = pl.BlockSpec(memory_space=pl.ANY)
DMA = pltpu.SemaphoreType.DMA


def shards(grads, momentum, basis):
    steps = COLS // STEP
    full, turned, blended = pl.pallas_call(
        blend_kernel,
        out_shape=(shape((4, 4, 4, SLICE, RANK)), shape((4, 4, PIECE, ROWS)), shape((2, ROWS, COLS))),
        in_specs=[ANY] * 3,
        out_specs=(VM, VM, VM),
        scratch_shapes=[
            pltpu.VMEM((ROWS, COLS), BF16),
            pltpu.VMEM((ROWS, COLS), BF16),
            pltpu.VMEM((ROWS, COLS), BF16),
            pltpu.VMEM((COLS, RANK), BF16),
            pltpu.VMEM((ROWS, RANK), F32),
            pltpu.VMEM((COLS, ROWS), BF16),
            pltpu.VMEM((3, SLICE, RANK), BF16),
            pltpu.VMEM((3, SLICE, RANK), BF16),
            DMA((3, steps)),
            DMA((steps,)),
            DMA((steps,)),
            DMA((3,)),
            DMA((3,)),
            DMA((3, 3, 4)),
            DMA((3, 3, 4)),
            DMA((16,)),
            DMA((16,)),
            DMA((1,)),
            DMA((1,)),
        ],
        compiler_params=pltpu.CompilerParams(has_side_effects=True),
        name="blend",
    )(grads, momentum, basis)
    own, back, squares = pl.pallas_call(
        basis_kernel,
        out_shape=(shape((ROWS, RANK)), shape((PIECE, RANK)), shape((8, RANK), F32)),
        in_specs=[VM] * 2,
        out_specs=(VM, VM, VM),
        scratch_shapes=[
            pltpu.VMEM((RANK, RANK), F32),
            pltpu.VMEM((RANK, RANK), F32),
            pltpu.VMEM((BLOCK, 2 * BLOCK), F32),
            pltpu.VMEM((BLOCK, BLOCK), F32),
            pltpu.VMEM((PIECE, RANK), F32),
        ],
        name="left_basis",
    )(full.reshape(16, ROWS, RANK), turned.reshape(16, PIECE, ROWS))
    gathered, norms, left = pl.pallas_call(
        gather_kernel,
        out_shape=(shape((2, 4, 4, PIECE, RANK)), shape((2, 8, RANK), F32), shape((2, ROWS, RANK))),
        in_specs=[VM] * 3,
        out_specs=(VM, VM, VM),
        scratch_shapes=[
            pltpu.VMEM((3, 4, 8, RANK), F32),
            DMA((2, 2, 4)),
            DMA((2, 2, 4)),
            DMA((3, 3)),
            DMA((3, 3)),
            DMA((10,)),
            DMA((10,)),
            DMA((2,)),
        ],
        compiler_params=pltpu.CompilerParams(has_side_effects=True),
        name="gather",
    )(back, squares, own)
    wide = COLS // 4
    return pl.pallas_call(
        output_kernel,
        out_shape=(shape((2, ROWS, COLS)), shape((2, ROWS, COLS)), shape((2, COLS, RANK))),
        grid=(2, 4),
        in_specs=[
            pl.BlockSpec((1, ROWS, RANK), lambda w, c: (w, 0, 0)),
            pl.BlockSpec((1, wide, RANK), lambda w, c: (w, c, 0)),
            pl.BlockSpec((1, ROWS, wide), lambda w, c: (w, 0, c)),
            pl.BlockSpec((1, 8, RANK), lambda w, c: (w, 0, 0)),
        ],
        out_specs=(
            pl.BlockSpec((1, ROWS, wide), lambda w, c: (w, 0, c)),
            pl.BlockSpec((1, ROWS, wide), lambda w, c: (w, 0, c)),
            pl.BlockSpec((1, wide, RANK), lambda w, c: (w, c, 0)),
        ),
        name="outputs",
    )(left, gathered.reshape(2, COLS, RANK), blended, norms)


def solution(mesh):
    torus = Mesh(
        mesh.devices.reshape(mesh.shape["replica"], 4, 4, mesh.shape["tensor"]),
        ("replica", "fsdp_0", "fsdp_1", "tensor"),
    )
    return jax.shard_map(
        shards,
        mesh=torus,
        in_specs=(
            P("replica", None, FSDP, "tensor"),
            P(None, FSDP, "tensor"),
            P(None, "tensor", None),
        ),
        out_specs=(P(None, FSDP, "tensor"), P(None, FSDP, "tensor"), P(None, "tensor", None)),
        check_vma=False,
    )
```

```python
import functools
import math

import jax
import jax.numpy as jnp
from jax import lax
from jax.experimental import pallas as pl
from jax.experimental.pallas import tpu as pltpu
from jax.sharding import Mesh
from jax.sharding import PartitionSpec as P

FEATURES = 4096
UNITS = 14336
RANK = 512
FSDP = ("fsdp_0", "fsdp_1")
MESH = pl.DeviceIdType.MESH
BF16 = jnp.bfloat16
F32 = jnp.float32
ROWS = FEATURES // 16
COLS = UNITS // 4
PIECE = COLS // 16
SLICE = ROWS // 4
STEP = 512
PANEL = 16
BLOCK = 128

momentum_decay = 0.95


def coords():
    return tuple(lax.axis_index(a) for a in ("replica", "fsdp_0", "fsdp_1", "tensor"))


def shifted(i, k):
    return lax.rem(i + k, 4)


class Ring:
    def __init__(self, axis, at, send, recv):
        self.axis, self.at, self.send, self.recv = axis, at, send, recv
        me = lax.axis_index(axis)
        self.me, self.right, self.left, self.far = me, shifted(me, 1), shifted(me, 3), shifted(me, 2)

    def copy(self, k, who, half, to):
        ref = self.at(who, half)
        return pltpu.make_async_remote_copy(
            src_ref=ref,
            dst_ref=ref,
            send_sem=self.send.at[k],
            recv_sem=self.recv.at[k],
            device_id={self.axis: to},
            device_id_type=MESH,
        )

    def start(self):
        self.copy(0, self.me, None, self.right).start()
        self.copy(1, self.me, None, self.left).start()

    def middle(self):
        self.copy(0, self.left, None, self.right).wait_recv()
        self.copy(2, self.left, 0, self.right).start()
        self.copy(1, self.right, None, self.left).wait_recv()
        self.copy(3, self.right, 1, self.left).start()

    def end(self):
        self.copy(2, self.far, 0, self.right).wait_recv()
        self.copy(3, self.far, 1, self.left).wait_recv()

    def drain(self):
        self.copy(0, self.me, None, self.right).wait_send()
        self.copy(1, self.me, None, self.left).wait_send()
        self.copy(2, self.left, 0, self.right).wait_send()
        self.copy(3, self.right, 1, self.left).wait_send()


def rows_of(start, size, half):
    if half is None:
        return pl.ds(start, size)
    return pl.ds(start + half * (size // 2), size // 2)


def projected_rings(full, y, x, z, send, recv):
    parts = ((0, 32, 0, 384), (32, 32, 0, 384), (0, 64, 384, 128))

    def cut(part, half):
        r0, nr, c0, nc = parts[part]
        return rows_of(r0, nr, half), pl.ds(c0, nc)

    every = slice(None)
    plans = (
        (0, 0, "tensor", lambda i: (y, x, i)),
        (0, 1, "fsdp_0", lambda i: (i, x, every)),
        (0, 2, "fsdp_1", lambda i: (every, i, every)),
        (1, 0, "fsdp_1", lambda i: (y, i, z)),
        (1, 1, "tensor", lambda i: (y, every, i)),
        (1, 2, "fsdp_0", lambda i: (i, every, every)),
        (2, 0, "fsdp_0", lambda i: (i, x, z)),
        (2, 1, "fsdp_1", lambda i: (every, i, z)),
        (2, 2, "tensor", lambda i: (every, every, i)),
    )
    phases = ([], [], [])
    for part, phase, axis, where in plans:
        def at(i, half, part=part, where=where):
            return full.at[(*where(i), *cut(part, half))]

        phases[phase].append(Ring(axis, at, send.at[part, phase], recv.at[part, phase]))
    return phases


class Spread:
    def __init__(self, part, r, y, x, held, out, send, recv, store):
        self.part, self.r, self.held, self.out, self.store = part, r, held, out, store
        self.send, self.recv = send.at[part], recv.at[part]
        self.line_axis, self.side_axis = ("fsdp_0", "fsdp_1") if part == 0 else ("fsdp_1", "fsdp_0")
        self.a, self.b = (y, x) if part == 0 else (x, y)
        self.sent = []
        self.stored = []

    def ref(self, o, q, half=None):
        i, j = shifted(self.a, o), shifted(self.b, q)
        place = (i, j) if self.part == 0 else (j, i)
        return (*place, rows_of(0, PIECE, half), pl.ds(self.part * (RANK // 2), RANK // 2))

    def copy(self, k, o, q, axis, way, half=None):
        ref = self.held.at[self.ref(o, q, half)]
        return pltpu.make_async_remote_copy(
            src_ref=ref,
            dst_ref=ref,
            send_sem=self.send.at[k],
            recv_sem=self.recv.at[k],
            device_id={axis: shifted(lax.axis_index(axis), way)},
            device_id_type=MESH,
        )

    def go(self, *args):
        copy = self.copy(*args)
        copy.start()
        self.sent.append(copy)

    def hand_over(self, o, q):
        k = 16 + 4 * o + q
        ref = self.ref(o, q)
        copy = pltpu.make_async_remote_copy(
            src_ref=self.held.at[ref],
            dst_ref=self.out.at[(self.r, *ref)],
            send_sem=self.send.at[k],
            recv_sem=self.recv.at[k],
            device_id={"replica": 1 - self.r},
            device_id_type=MESH,
        )
        copy.start()
        self.sent.append(copy)
        kept = pltpu.make_async_copy(
            self.held.at[ref], self.out.at[(self.r, *ref)], self.store.at[3 + 16 * self.part + 4 * o + q]
        )
        kept.start()
        self.stored.append(kept)

    def begin(self):
        self.go(0, 0, 0, self.line_axis, 1)
        self.go(1, 0, 0, self.line_axis, 3)
        self.sides(0)
        self.hand_over(0, 0)

    def sides(self, o):
        self.go(4 + o, o, 0, self.side_axis, 1)
        self.go(8 + o, o, 0, self.side_axis, 3)

    def line(self, o):
        if o == 3:
            self.copy(0, 3, 0, self.line_axis, 1).wait_recv()
            self.go(2, 3, 0, self.line_axis, 1, 0)
        elif o == 1:
            self.copy(1, 1, 0, self.line_axis, 3).wait_recv()
            self.go(3, 1, 0, self.line_axis, 3, 1)
        else:
            self.copy(2, 2, 0, self.line_axis, 1, 0).wait_recv()
            self.copy(3, 2, 0, self.line_axis, 3, 1).wait_recv()
        self.sides(o)
        self.hand_over(o, 0)

    def side(self, o):
        first, second = ((3, 1) if o in (0, 3) else (1, 3))
        for q in (first, second):
            if q == 3:
                self.copy(4 + o, o, 3, self.side_axis, 1).wait_recv()
            else:
                self.copy(8 + o, o, 1, self.side_axis, 3).wait_recv()
            if q == first:
                self.go(12 + o, o, q, self.side_axis, 4 - q)
            self.hand_over(o, q)

    def last(self, o):
        self.copy(12 + o, o, 2, self.side_axis, 1 if o in (0, 3) else 3).wait_recv()
        self.hand_over(o, 2)

    def drain(self):
        for copy in self.sent:
            copy.wait_send()
        for copy in self.stored:
            copy.wait()
        for o in range(4):
            for q in range(4):
                k = 16 + 4 * o + q
                ref = self.out.at[(1 - self.r, *self.ref(o, q))]
                pltpu.make_async_remote_copy(
                    src_ref=ref,
                    dst_ref=ref,
                    send_sem=self.send.at[k],
                    recv_sem=self.recv.at[k],
                    device_id={"replica": 1 - self.r},
                    device_id_type=MESH,
                ).wait_recv()


def halves(value):
    high = value.astype(BF16)
    return high, (value - high.astype(F32)).astype(BF16)


def contract_rows(a, b):
    ah, al = halves(a)
    bh, bl = halves(b)
    return lax.dot_general(
        jnp.concatenate([ah, ah, al], axis=0),
        jnp.concatenate([bh, bl, bh], axis=0),
        (((0,), (0,)), ((), ())),
        preferred_element_type=F32,
    )


def product(a, b):
    ah, al = halves(a)
    bh, bl = halves(b)
    return jnp.dot(
        jnp.concatenate([ah, ah, al], axis=1),
        jnp.concatenate([bh, bl, bh], axis=0),
        preferred_element_type=F32,
    )


def eliminate(work, inverse):
    row = lax.broadcasted_iota(jnp.int32, (PANEL, BLOCK), 0)
    lane = lax.broadcasted_iota(jnp.int32, (BLOCK, BLOCK), 1)

    def panel(p, carry):
        left, right = work[0:PANEL, 0:BLOCK], work[0:PANEL, BLOCK:]
        columns = [jnp.broadcast_to(left[:, k : k + 1], (PANEL, BLOCK)) for k in range(PANEL)]
        inverses = jnp.ones((PANEL, BLOCK), F32)
        for j in range(PANEL):
            inv = 1.0 / columns[j][j : j + 1, :]
            times = jnp.where(row > j, columns[j] * inv, 0.0)
            for k in range(j + 1, PANEL):
                columns[k] = columns[k] - times * columns[k][j : j + 1, :]
            left = left - times * left[j : j + 1, :]
            right = right - times * right[j : j + 1, :]
            inverses = jnp.where(row == j, inv, inverses)
        scale = jnp.sqrt(inverses)
        left, right = left * scale, right * scale
        inverse[pl.ds(pl.multiple_of(p * PANEL, PANEL), PANEL), :] = right
        change = contract_rows(left, jnp.concatenate([left, right], axis=1))
        rest = work[:, 0:BLOCK] - change[:, 0:BLOCK]
        rest = jnp.where(lane < BLOCK - PANEL, pltpu.roll(rest, BLOCK - PANEL, 1), 0.0)
        work[0 : BLOCK - PANEL, 0:BLOCK] = rest[PANEL:, :]
        extra = work[:, BLOCK:] - change[:, BLOCK:]
        work[0 : BLOCK - PANEL, BLOCK:] = extra[PANEL:, :]
        work[BLOCK - PANEL :, :] = jnp.zeros((PANEL, 2 * BLOCK), F32)
        return carry

    lax.fori_loop(0, BLOCK // PANEL, panel, 0)


def factor_inverse(gram, low, work, inverse):
    low[...] = jnp.zeros_like(low)
    count = RANK // BLOCK
    square = (BLOCK, BLOCK)
    eye = jnp.where(
        lax.broadcasted_iota(jnp.int32, square, 0) == lax.broadcasted_iota(jnp.int32, square, 1), 1.0, 0.0
    )
    for k in range(count):
        here, after = slice(k * BLOCK, (k + 1) * BLOCK), slice((k + 1) * BLOCK, RANK)
        work[:, 0:BLOCK] = gram[here, here]
        work[:, BLOCK:] = eye
        eliminate(work, inverse)
        block = inverse[...]
        if k:
            low[here, 0 : k * BLOCK] = product(block, low[here, 0 : k * BLOCK])
        low[here, here] = block
        if k < count - 1:
            upper = product(block, gram[here, after])
            gram[after, after] = gram[after, after] - contract_rows(upper, upper)
            done = slice(0, (k + 1) * BLOCK)
            low[after, done] = low[after, done] - contract_rows(upper, low[here, done])


def step_kernel(
    grads, momentum, basis, blended, gathered, norms, left,
    m_v, g_v, gp_v, b_v, acc, flipped, out_z, in_z, full, turned, gram, low, work, inverse, total, own, rows_v, sums,
    load, gs, gr, zs, zr, ags, agr, ts, tr, bs, br, s_n, r_n, s_p, r_p, store,
):
    r, y, x, z = coords()
    other = 1 - r
    steps = COLS // STEP

    def grad_copy(c, cols):
        return pltpu.make_async_remote_copy(
            src_ref=grads.at[0, other, :, cols],
            dst_ref=gp_v.at[:, cols],
            send_sem=gs.at[c],
            recv_sem=gr.at[c],
            device_id={"replica": other},
            device_id_type=MESH,
        )

    def loads(c, cols):
        return (
            pltpu.make_async_copy(grads.at[0, r, :, cols], g_v.at[:, cols], load.at[0, c]),
            pltpu.make_async_copy(momentum.at[r, :, cols], m_v.at[:, cols], load.at[1, c]),
            pltpu.make_async_copy(basis.at[r, cols, :], b_v.at[cols, :], load.at[2, c]),
        )

    for c in range(steps):
        cols = pl.ds(c * STEP, STEP)
        grad_copy(c, cols).start()
        for copy in loads(c, cols):
            copy.start()
    acc[...] = jnp.zeros_like(acc)

    def blend(c, carry):
        cols = pl.ds(pl.multiple_of(c * STEP, STEP), STEP)
        for copy in loads(c, cols):
            copy.wait()
        grad_copy(c, cols).wait()
        both = g_v[:, cols].astype(F32) + gp_v[:, cols].astype(F32)
        value = (m_v[:, cols].astype(F32) + both).astype(BF16)
        m_v[:, cols] = value
        acc[...] += jnp.dot(value, b_v[cols, :], preferred_element_type=F32)
        return carry

    lax.fori_loop(0, steps, blend, 0)

    def z_copy(k):
        return pltpu.make_async_remote_copy(
            src_ref=out_z.at[k - 1],
            dst_ref=in_z.at[k - 1],
            send_sem=zs.at[k - 1],
            recv_sem=zr.at[k - 1],
            device_id={"tensor": shifted(z, k)},
            device_id_type=MESH,
        )

    for k in (2, 1, 3):
        rows = pl.ds(pl.multiple_of(shifted(z, k) * SLICE, SLICE), SLICE)
        out_z[k - 1] = acc[rows, :].astype(BF16)
        z_copy(k).start()

    def flip(c, carry):
        cols = pl.ds(pl.multiple_of(c * STEP, STEP), STEP)
        flipped[cols, :] = m_v[:, cols].T
        return carry

    lax.fori_loop(0, steps, flip, 0)
    piece = acc[pl.ds(pl.multiple_of(z * SLICE, SLICE), SLICE), :]
    for k in (1, 3, 2):
        z_copy(k).wait()
        piece = piece + in_z[k - 1].astype(F32)
    full[y, x, z] = piece.astype(BF16)

    phases = projected_rings(full, y, x, z, ags, agr)
    for phase in phases:
        for ring in phase:
            ring.start()
        for ring in phase:
            ring.middle()
        if phase is not phases[-1]:
            for ring in phase:
                ring.end()

    def turn_copy(k):
        ty, tx = shifted(y, k // 4), shifted(x, k % 4)
        start = pl.multiple_of((ty * 4 + tx) * PIECE, PIECE)
        return pltpu.make_async_remote_copy(
            src_ref=flipped.at[pl.ds(start, PIECE), :],
            dst_ref=turned.at[y, x],
            send_sem=ts.at[k],
            recv_sem=tr.at[k],
            device_id={"fsdp_0": ty, "fsdp_1": tx},
            device_id_type=MESH,
        )

    def turn_arrival(k):
        sy, sx = shifted(y, 4 - k // 4), shifted(x, 4 - k % 4)
        return pltpu.make_async_remote_copy(
            src_ref=turned.at[sy, sx],
            dst_ref=turned.at[sy, sx],
            send_sem=ts.at[k],
            recv_sem=tr.at[k],
            device_id={"fsdp_0": sy, "fsdp_1": sx},
            device_id_type=MESH,
        )

    for k in range(1, 16):
        turn_copy(k).start()

    def to_partner(src, dst, send, recv):
        return pltpu.make_async_remote_copy(
            src_ref=src,
            dst_ref=dst,
            send_sem=send,
            recv_sem=recv,
            device_id={"replica": other},
            device_id_type=MESH,
        )

    share = to_partner(m_v, blended.at[r], bs.at[0], br.at[0])
    share.start()
    keep = pltpu.make_async_copy(m_v, blended.at[r], store.at[0])
    keep.start()
    turned[y, x] = flipped[pl.ds(pl.multiple_of((y * 4 + x) * PIECE, PIECE), PIECE), :]
    for ring in phases[-1]:
        ring.end()

    gram[...] = jnp.zeros_like(gram)

    def add_gram(b, carry):
        rows = full[b // 4, lax.rem(b, 4)].reshape(ROWS, RANK)
        gram[...] += lax.dot_general(rows, rows, (((0,), (0,)), ((), ())), preferred_element_type=F32)
        return carry

    lax.fori_loop(0, 16, add_gram, 0)
    factor_inverse(gram, low, work, inverse)
    high = low[...].astype(BF16)
    total[...] = jnp.zeros_like(total)
    dims = (((1,), (1,)), ((), ()))

    def left_rows(by, bx):
        rows = full[by, bx].reshape(ROWS, RANK)
        return lax.dot_general(rows, high, dims, preferred_element_type=F32).astype(BF16)

    own[...] = left_rows(y, x)
    keep_left = pltpu.make_async_copy(own, left.at[r], store.at[1])
    keep_left.start()
    share_left = to_partner(own, left.at[r], bs.at[1], br.at[1])
    share_left.start()
    for k in range(1, 16):
        turn_copy(k).wait_send()
        turn_arrival(k).wait_recv()

    def add_back(b, carry):
        by, bx = b // 4, lax.rem(b, 4)
        total[...] += jnp.dot(turned[by, bx], left_rows(by, bx), preferred_element_type=F32)
        return carry

    lax.fori_loop(0, 16, add_back, 0)
    value = total[...]
    rows_v[y, x] = value.astype(BF16)

    def sum_copy(phase, axis, k, me):
        return pltpu.make_async_remote_copy(
            src_ref=sums.at[phase, me],
            dst_ref=sums.at[phase, me],
            send_sem=s_n.at[phase, k - 1],
            recv_sem=r_n.at[phase, k - 1],
            device_id={axis: shifted(me, k)},
            device_id_type=MESH,
        )

    def sum_arrival(phase, axis, k, me):
        source = shifted(me, 4 - k)
        return pltpu.make_async_remote_copy(
            src_ref=sums.at[phase, source],
            dst_ref=sums.at[phase, source],
            send_sem=s_n.at[phase, k - 1],
            recv_sem=r_n.at[phase, k - 1],
            device_id={axis: source},
            device_id_type=MESH,
        )

    def send_sums(phase, axis, me, block):
        sums[phase, me] = block
        for k in (2, 1, 3):
            sum_copy(phase, axis, k, me).start()

    def take_sums(phase, axis, me):
        for k in (1, 3, 2):
            sum_arrival(phase, axis, k, me).wait_recv()
        return (sums[phase, 0] + sums[phase, 1]) + (sums[phase, 2] + sums[phase, 3])

    spreads = (Spread(0, r, y, x, rows_v, gathered, s_p, r_p, store), Spread(1, r, y, x, rows_v, gathered, s_p, r_p, store))

    def both(job, *args):
        for spread in spreads:
            getattr(spread, job)(*args)

    both("begin")
    send_sums(0, "tensor", z, jnp.sum((value * value).reshape(PIECE // 8, 8, RANK), axis=0))
    both("line", 3)
    both("line", 1)
    part_sums = take_sums(0, "tensor", z)
    send_sums(1, "fsdp_1", x, part_sums)
    both("side", 0)
    both("line", 2)
    both("side", 3)
    part_sums = take_sums(1, "fsdp_1", x)
    send_sums(2, "fsdp_0", y, part_sums)
    both("side", 1)
    part_sums = take_sums(2, "fsdp_0", y)
    sums[3, 0] = part_sums
    keep_norms = pltpu.make_async_copy(sums.at[3, 0], norms.at[r], store.at[2])
    keep_norms.start()
    share_norms = to_partner(sums.at[3, 0], norms.at[r], bs.at[2], br.at[2])
    share_norms.start()
    both("side", 2)
    for sub in (0, 3, 1, 2):
        both("last", sub)
    both("drain")
    for ring in phases[0] + phases[1] + phases[2]:
        ring.drain()
    for phase, axis, me in ((0, "tensor", z), (1, "fsdp_1", x), (2, "fsdp_0", y)):
        for k in (1, 2, 3):
            sum_copy(phase, axis, k, me).wait_send()
    for copy in (keep, keep_left, keep_norms):
        copy.wait()
    for copy in (share, share_left, share_norms):
        copy.wait_send()
    for k, out in enumerate((blended, left, norms)):
        to_partner(out.at[other], out.at[other], bs.at[k], br.at[k]).wait_recv()


def output_kernel(left, back, blended, norms, momentum_new, update, basis_new):
    squares = jnp.sum(norms[0], axis=0, keepdims=True)
    inverse = 1.0 / (jnp.sqrt(squares) + 1e-06)
    rows = back[0]
    normed = (rows.astype(F32) * inverse).astype(BF16)
    basis_new[0] = normed
    dims = (((1,), (1,)), ((), ()))
    feedback = lax.dot_general(left[0], rows, dims, preferred_element_type=F32)
    momentum_new[0] = (blended[0].astype(F32) - (1.0 - momentum_decay) * feedback).astype(BF16)
    scale = math.sqrt(FEATURES * UNITS / RANK)
    update[0] = (scale * lax.dot_general(left[0], normed, dims, preferred_element_type=F32)).astype(BF16)


def shape(dims, dtype=BF16):
    return jax.ShapeDtypeStruct(dims, dtype)


VM = pl.BlockSpec(memory_space=pltpu.VMEM)
ANY = pl.BlockSpec(memory_space=pl.ANY)
DMA = pltpu.SemaphoreType.DMA


def shards(grads, momentum, basis):
    steps = COLS // STEP
    blended, gathered, norms, left = pl.pallas_call(
        step_kernel,
        out_shape=(
            shape((2, ROWS, COLS)),
            shape((2, 4, 4, PIECE, RANK)),
            shape((2, 8, RANK), F32),
            shape((2, ROWS, RANK)),
        ),
        in_specs=[ANY] * 3,
        out_specs=(ANY,) * 4,
        scratch_shapes=[
            pltpu.VMEM((ROWS, COLS), BF16),
            pltpu.VMEM((ROWS, COLS), BF16),
            pltpu.VMEM((ROWS, COLS), BF16),
            pltpu.VMEM((COLS, RANK), BF16),
            pltpu.VMEM((ROWS, RANK), F32),
            pltpu.VMEM((COLS, ROWS), BF16),
            pltpu.VMEM((3, SLICE, RANK), BF16),
            pltpu.VMEM((3, SLICE, RANK), BF16),
            pltpu.VMEM((4, 4, 4, SLICE, RANK), BF16),
            pltpu.VMEM((4, 4, PIECE, ROWS), BF16),
            pltpu.VMEM((RANK, RANK), F32),
            pltpu.VMEM((RANK, RANK), F32),
            pltpu.VMEM((BLOCK, 2 * BLOCK), F32),
            pltpu.VMEM((BLOCK, BLOCK), F32),
            pltpu.VMEM((PIECE, RANK), F32),
            pltpu.VMEM((ROWS, RANK), BF16),
            pltpu.VMEM((4, 4, PIECE, RANK), BF16),
            pltpu.VMEM((4, 4, 8, RANK), F32),
            DMA((3, steps)),
            DMA((steps,)),
            DMA((steps,)),
            DMA((3,)),
            DMA((3,)),
            DMA((3, 3, 4)),
            DMA((3, 3, 4)),
            DMA((16,)),
            DMA((16,)),
            DMA((3,)),
            DMA((3,)),
            DMA((3, 3)),
            DMA((3, 3)),
            DMA((2, 32)),
            DMA((2, 32)),
            DMA((35,)),
        ],
        compiler_params=pltpu.CompilerParams(has_side_effects=True),
        name="step",
    )(grads, momentum, basis)
    wide = COLS // 4
    return pl.pallas_call(
        output_kernel,
        out_shape=(shape((2, ROWS, COLS)), shape((2, ROWS, COLS)), shape((2, COLS, RANK))),
        grid=(2, 4),
        in_specs=[
            pl.BlockSpec((1, ROWS, RANK), lambda w, c: (w, 0, 0)),
            pl.BlockSpec((1, wide, RANK), lambda w, c: (w, c, 0)),
            pl.BlockSpec((1, ROWS, wide), lambda w, c: (w, 0, c)),
            pl.BlockSpec((1, 8, RANK), lambda w, c: (w, 0, 0)),
        ],
        out_specs=(
            pl.BlockSpec((1, ROWS, wide), lambda w, c: (w, 0, c)),
            pl.BlockSpec((1, ROWS, wide), lambda w, c: (w, 0, c)),
            pl.BlockSpec((1, wide, RANK), lambda w, c: (w, c, 0)),
        ),
        name="outputs",
    )(left, gathered.reshape(2, COLS, RANK), blended, norms)


def solution(mesh):
    torus = Mesh(
        mesh.devices.reshape(mesh.shape["replica"], 4, 4, mesh.shape["tensor"]),
        ("replica", "fsdp_0", "fsdp_1", "tensor"),
    )
    return jax.shard_map(
        shards,
        mesh=torus,
        in_specs=(
            P("replica", None, FSDP, "tensor"),
            P(None, FSDP, "tensor"),
            P(None, "tensor", None),
        ),
        out_specs=(P(None, FSDP, "tensor"), P(None, FSDP, "tensor"), P(None, "tensor", None)),
        check_vma=False,
    )
```

```python
import functools
import math

import jax
import jax.numpy as jnp
from jax import lax
from jax.experimental import pallas as pl
from jax.experimental.pallas import tpu as pltpu
from jax.sharding import Mesh
from jax.sharding import PartitionSpec as P

FEATURES = 4096
UNITS = 14336
RANK = 512
FSDP = ("fsdp_0", "fsdp_1")
MESH = pl.DeviceIdType.MESH
BF16 = jnp.bfloat16
F32 = jnp.float32
ROWS = FEATURES // 16
COLS = UNITS // 4
PIECE = COLS // 16
SLICE = ROWS // 4
STEP = 512
PANEL = 16
BLOCK = 128
CHUNKS = 4

momentum_decay = 0.95


def coords():
    return tuple(lax.axis_index(a) for a in ("replica", "fsdp_0", "fsdp_1", "tensor"))


def shifted(i, k):
    return lax.rem(i + k, 4)


class Ring:
    def __init__(self, axis, at, send, recv):
        self.axis, self.at, self.send, self.recv = axis, at, send, recv
        me = lax.axis_index(axis)
        self.me, self.right, self.left, self.far = me, shifted(me, 1), shifted(me, 3), shifted(me, 2)

    def copy(self, k, who, half, to):
        ref = self.at(who, half)
        return pltpu.make_async_remote_copy(
            src_ref=ref,
            dst_ref=ref,
            send_sem=self.send.at[k],
            recv_sem=self.recv.at[k],
            device_id={self.axis: to},
            device_id_type=MESH,
        )

    def start(self):
        self.copy(0, self.me, None, self.right).start()
        self.copy(1, self.me, None, self.left).start()

    def middle(self):
        self.copy(0, self.left, None, self.right).wait_recv()
        self.copy(2, self.left, 0, self.right).start()
        self.copy(1, self.right, None, self.left).wait_recv()
        self.copy(3, self.right, 1, self.left).start()

    def end(self):
        self.copy(2, self.far, 0, self.right).wait_recv()
        self.copy(3, self.far, 1, self.left).wait_recv()

    def drain(self):
        self.copy(0, self.me, None, self.right).wait_send()
        self.copy(1, self.me, None, self.left).wait_send()
        self.copy(2, self.left, 0, self.right).wait_send()
        self.copy(3, self.right, 1, self.left).wait_send()


def rows_of(start, size, half):
    if half is None:
        return pl.ds(start, size)
    return pl.ds(start + half * (size // 2), size // 2)


def projected_gather(full, y, x, z, send, recv):
    parts = ((0, 32, 0, 384), (32, 32, 0, 384), (0, 64, 384, 128))

    def cut(part, half):
        r0, nr, c0, nc = parts[part]
        return rows_of(r0, nr, half), pl.ds(c0, nc)

    every = slice(None)
    plans = (
        ("tensor", "fsdp_0", "fsdp_1", lambda i: (y, x, i), lambda o, q: (shifted(y, o), shifted(x, q), every)),
        ("fsdp_1", "tensor", "fsdp_0", lambda i: (y, i, z), lambda o, q: (shifted(y, q), every, shifted(z, o))),
        ("fsdp_0", "fsdp_1", "tensor", lambda i: (i, x, z), lambda o, q: (every, shifted(x, o), shifted(z, q))),
    )
    rings, spreads = [], []
    for part, (first, line, side, ring_at, spread_at) in enumerate(plans):
        def at_ring(i, half, part=part, where=ring_at):
            return full.at[(*where(i), *cut(part, half))]

        def at_spread(o, q, half, part=part, where=spread_at):
            return full.at[(*where(o, q), *cut(part, half))]

        rings.append(Ring(first, at_ring, send.at[part, 0], recv.at[part, 0]))
        spreads.append(Spread(at_spread, line, side, send.at[part, 1], recv.at[part, 1]))
    return rings, spreads


class Spread:
    def __init__(self, at, line_axis, side_axis, send, recv, hand=None):
        self.at, self.send, self.recv = at, send, recv
        self.line_axis, self.side_axis = line_axis, side_axis
        self.hand = hand or (lambda o, q: None)
        self.sent = []

    def copy(self, k, o, q, axis, way, half=None):
        ref = self.at(o, q, half)
        return pltpu.make_async_remote_copy(
            src_ref=ref,
            dst_ref=ref,
            send_sem=self.send.at[k],
            recv_sem=self.recv.at[k],
            device_id={axis: shifted(lax.axis_index(axis), way)},
            device_id_type=MESH,
        )

    def go(self, *args):
        copy = self.copy(*args)
        copy.start()
        self.sent.append(copy)

    def begin(self):
        self.go(0, 0, 0, self.line_axis, 1)
        self.go(1, 0, 0, self.line_axis, 3)
        self.sides(0)
        self.hand(0, 0)

    def sides(self, o):
        self.go(4 + o, o, 0, self.side_axis, 1)
        self.go(8 + o, o, 0, self.side_axis, 3)

    def line(self, o):
        if o == 3:
            self.copy(0, 3, 0, self.line_axis, 1).wait_recv()
            self.go(2, 3, 0, self.line_axis, 1, 0)
        elif o == 1:
            self.copy(1, 1, 0, self.line_axis, 3).wait_recv()
            self.go(3, 1, 0, self.line_axis, 3, 1)
        else:
            self.copy(2, 2, 0, self.line_axis, 1, 0).wait_recv()
            self.copy(3, 2, 0, self.line_axis, 3, 1).wait_recv()
        self.sides(o)
        self.hand(o, 0)

    def side(self, o):
        first, second = (3, 1) if o in (0, 3) else (1, 3)
        for q in (first, second):
            if q == 3:
                self.copy(4 + o, o, 3, self.side_axis, 1).wait_recv()
            else:
                self.copy(8 + o, o, 1, self.side_axis, 3).wait_recv()
            if q == first:
                self.go(12 + o, o, q, self.side_axis, 4 - q)
            self.hand(o, q)

    def last(self, o):
        self.copy(12 + o, o, 2, self.side_axis, 1 if o in (0, 3) else 3).wait_recv()
        self.hand(o, 2)

    def drain(self):
        for copy in self.sent:
            copy.wait_send()


SPREAD_STEPS = (("line", 3), ("line", 1), ("side", 0), ("line", 2), ("side", 3), ("side", 1), ("side", 2))


def together(spreads, job, *args):
    for spread in spreads:
        getattr(spread, job)(*args)


def halves(value):
    high = value.astype(BF16)
    return high, (value - high.astype(F32)).astype(BF16)


def contract_rows(a, b):
    ah, al = halves(a)
    bh, bl = halves(b)
    return lax.dot_general(
        jnp.concatenate([ah, ah, al], axis=0),
        jnp.concatenate([bh, bl, bh], axis=0),
        (((0,), (0,)), ((), ())),
        preferred_element_type=F32,
    )


def product(a, b):
    ah, al = halves(a)
    bh, bl = halves(b)
    return jnp.dot(
        jnp.concatenate([ah, ah, al], axis=1),
        jnp.concatenate([bh, bl, bh], axis=0),
        preferred_element_type=F32,
    )


def eliminate(work, inverse):
    row = lax.broadcasted_iota(jnp.int32, (PANEL, BLOCK), 0)
    lane = lax.broadcasted_iota(jnp.int32, (BLOCK, BLOCK), 1)

    def panel(p, carry):
        left, right = work[0:PANEL, 0:BLOCK], work[0:PANEL, BLOCK:]
        columns = [jnp.broadcast_to(left[:, k : k + 1], (PANEL, BLOCK)) for k in range(PANEL)]
        inverses = jnp.ones((PANEL, BLOCK), F32)
        for j in range(PANEL):
            inv = 1.0 / columns[j][j : j + 1, :]
            times = jnp.where(row > j, columns[j] * inv, 0.0)
            for k in range(j + 1, PANEL):
                columns[k] = columns[k] - times * columns[k][j : j + 1, :]
            left = left - times * left[j : j + 1, :]
            right = right - times * right[j : j + 1, :]
            inverses = jnp.where(row == j, inv, inverses)
        scale = jnp.sqrt(inverses)
        left, right = left * scale, right * scale
        inverse[pl.ds(pl.multiple_of(p * PANEL, PANEL), PANEL), :] = right
        change = contract_rows(left, jnp.concatenate([left, right], axis=1))
        rest = work[:, 0:BLOCK] - change[:, 0:BLOCK]
        rest = jnp.where(lane < BLOCK - PANEL, pltpu.roll(rest, BLOCK - PANEL, 1), 0.0)
        work[0 : BLOCK - PANEL, 0:BLOCK] = rest[PANEL:, :]
        extra = work[:, BLOCK:] - change[:, BLOCK:]
        work[0 : BLOCK - PANEL, BLOCK:] = extra[PANEL:, :]
        work[BLOCK - PANEL :, :] = jnp.zeros((PANEL, 2 * BLOCK), F32)
        return carry

    lax.fori_loop(0, BLOCK // PANEL, panel, 0)


def factor_inverse(gram, low, work, inverse):
    low[...] = jnp.zeros_like(low)
    count = RANK // BLOCK
    square = (BLOCK, BLOCK)
    eye = jnp.where(
        lax.broadcasted_iota(jnp.int32, square, 0) == lax.broadcasted_iota(jnp.int32, square, 1), 1.0, 0.0
    )
    for k in range(count):
        here, after = slice(k * BLOCK, (k + 1) * BLOCK), slice((k + 1) * BLOCK, RANK)
        work[:, 0:BLOCK] = gram[here, here]
        work[:, BLOCK:] = eye
        eliminate(work, inverse)
        block = inverse[...]
        if k:
            low[here, 0 : k * BLOCK] = product(block, low[here, 0 : k * BLOCK])
        low[here, here] = block
        if k < count - 1:
            upper = product(block, gram[here, after])
            gram[after, after] = gram[after, after] - contract_rows(upper, upper)
            done = slice(0, (k + 1) * BLOCK)
            low[after, done] = low[after, done] - contract_rows(upper, low[here, done])


def step_kernel(
    grads, momentum, basis, blended, gathered, norms, left,
    m_v, g_v, gp_v, b_v, acc, flipped, out_z, in_z, full, turned, gram, low, work, inverse, total, sums,
    load, gs, gr, zs, zr, ags, agr, ts, tr, bs, br, s_n, r_n, s_p, r_p,
):
    r, y, x, z = coords()
    other = 1 - r
    steps = COLS // STEP

    def grad_copy(c, cols):
        return pltpu.make_async_remote_copy(
            src_ref=grads.at[0, other, :, cols],
            dst_ref=gp_v.at[:, cols],
            send_sem=gs.at[c],
            recv_sem=gr.at[c],
            device_id={"replica": other},
            device_id_type=MESH,
        )

    def loads(c, cols):
        return (
            pltpu.make_async_copy(grads.at[0, r, :, cols], g_v.at[:, cols], load.at[0, c]),
            pltpu.make_async_copy(momentum.at[r, :, cols], m_v.at[:, cols], load.at[1, c]),
            pltpu.make_async_copy(basis.at[r, cols, :], b_v.at[cols, :], load.at[2, c]),
        )

    for c in range(steps):
        cols = pl.ds(c * STEP, STEP)
        grad_copy(c, cols).start()
        for copy in loads(c, cols):
            copy.start()
    acc[...] = jnp.zeros_like(acc)

    def blend(c, carry):
        cols = pl.ds(pl.multiple_of(c * STEP, STEP), STEP)
        for copy in loads(c, cols):
            copy.wait()
        grad_copy(c, cols).wait()
        both = g_v[:, cols].astype(F32) + gp_v[:, cols].astype(F32)
        value = (m_v[:, cols].astype(F32) + both).astype(BF16)
        blended[r, :, cols] = value
        acc[...] += jnp.dot(value, b_v[cols, :], preferred_element_type=F32)
        return carry

    lax.fori_loop(0, steps, blend, 0)

    def z_copy(k):
        return pltpu.make_async_remote_copy(
            src_ref=out_z.at[k - 1],
            dst_ref=in_z.at[k - 1],
            send_sem=zs.at[k - 1],
            recv_sem=zr.at[k - 1],
            device_id={"tensor": shifted(z, k)},
            device_id_type=MESH,
        )

    for k in (2, 1, 3):
        rows = pl.ds(pl.multiple_of(shifted(z, k) * SLICE, SLICE), SLICE)
        out_z[k - 1] = acc[rows, :].astype(BF16)
        z_copy(k).start()

    def flip(c, carry):
        cols = pl.ds(pl.multiple_of(c * STEP, STEP), STEP)
        flipped[cols, :] = blended[r, :, cols].T
        return carry

    lax.fori_loop(0, steps, flip, 0)
    piece = acc[pl.ds(pl.multiple_of(z * SLICE, SLICE), SLICE), :]
    for k in (1, 3, 2):
        z_copy(k).wait()
        piece = piece + in_z[k - 1].astype(F32)
    full[y, x, z] = piece.astype(BF16)

    rings, wide = projected_gather(full, y, x, z, ags, agr)
    together(rings, "start")
    together(rings, "middle")
    together(rings, "end")
    together(wide, "begin")
    for job, o in SPREAD_STEPS:
        together(wide, job, o)

    def turn_copy(k):
        ty, tx = shifted(y, k // 4), shifted(x, k % 4)
        start = pl.multiple_of((ty * 4 + tx) * PIECE, PIECE)
        return pltpu.make_async_remote_copy(
            src_ref=flipped.at[pl.ds(start, PIECE), :],
            dst_ref=turned.at[y, x],
            send_sem=ts.at[k],
            recv_sem=tr.at[k],
            device_id={"fsdp_0": ty, "fsdp_1": tx},
            device_id_type=MESH,
        )

    def turn_arrival(k):
        sy, sx = shifted(y, 4 - k // 4), shifted(x, 4 - k % 4)
        return pltpu.make_async_remote_copy(
            src_ref=turned.at[sy, sx],
            dst_ref=turned.at[sy, sx],
            send_sem=ts.at[k],
            recv_sem=tr.at[k],
            device_id={"fsdp_0": sy, "fsdp_1": sx},
            device_id_type=MESH,
        )

    for k in range(1, 16):
        turn_copy(k).start()

    def to_partner(src, dst, send, recv):
        return pltpu.make_async_remote_copy(
            src_ref=src,
            dst_ref=dst,
            send_sem=send,
            recv_sem=recv,
            device_id={"replica": other},
            device_id_type=MESH,
        )

    share = to_partner(blended.at[r], blended.at[r], bs.at[0], br.at[0])
    share.start()
    turned[y, x] = flipped[pl.ds(pl.multiple_of((y * 4 + x) * PIECE, PIECE), PIECE), :]
    for o in (0, 3, 1, 2):
        together(wide, "last", o)

    gram[...] = jnp.zeros_like(gram)

    def add_gram(b, carry):
        rows = full[b].reshape(4 * ROWS, RANK)
        gram[...] += lax.dot_general(rows, rows, (((0,), (0,)), ((), ())), preferred_element_type=F32)
        return carry

    lax.fori_loop(0, 4, add_gram, 0)
    factor_inverse(gram, low, work, inverse)
    high = low[...].astype(BF16)
    total[...] = jnp.zeros_like(total)
    dims = (((1,), (1,)), ((), ()))

    def left_rows(rows):
        return lax.dot_general(rows, high, dims, preferred_element_type=F32).astype(BF16)

    for k in range(1, 16):
        turn_copy(k).wait_send()
        turn_arrival(k).wait_recv()

    def add_back(b, carry):
        rows = left_rows(full[b].reshape(4 * ROWS, RANK))
        for bx in range(4):
            total[...] += jnp.dot(turned[b, bx], rows[bx * ROWS : (bx + 1) * ROWS], preferred_element_type=F32)
        return carry

    lax.fori_loop(0, 4, add_back, 0)
    value = total[...]
    gathered[r, y, x] = value.astype(BF16)

    def sum_copy(phase, axis, k, me):
        return pltpu.make_async_remote_copy(
            src_ref=sums.at[phase, me],
            dst_ref=sums.at[phase, me],
            send_sem=s_n.at[phase, k - 1],
            recv_sem=r_n.at[phase, k - 1],
            device_id={axis: shifted(me, k)},
            device_id_type=MESH,
        )

    def sum_arrival(phase, axis, k, me):
        source = shifted(me, 4 - k)
        return pltpu.make_async_remote_copy(
            src_ref=sums.at[phase, source],
            dst_ref=sums.at[phase, source],
            send_sem=s_n.at[phase, k - 1],
            recv_sem=r_n.at[phase, k - 1],
            device_id={axis: source},
            device_id_type=MESH,
        )

    def send_sums(phase, axis, me, block):
        sums[phase, me] = block
        for k in (2, 1, 3):
            sum_copy(phase, axis, k, me).start()

    def take_sums(phase, axis, me):
        for k in (1, 3, 2):
            sum_arrival(phase, axis, k, me).wait_recv()
        return (sums[phase, 0] + sums[phase, 1]) + (sums[phase, 2] + sums[phase, 3])

    def spread_of(part):
        cols = pl.ds(part * (RANK // 2), RANK // 2)
        axes = ("fsdp_0", "fsdp_1") if part == 0 else ("fsdp_1", "fsdp_0")

        def place(o, q):
            return (shifted(y, o), shifted(x, q)) if part == 0 else (shifted(y, q), shifted(x, o))

        def at(o, q, half):
            return gathered.at[(r, *place(o, q), rows_of(0, PIECE, half), cols)]

        def passing(weight, o, q):
            ref = gathered.at[(weight, *place(o, q), slice(None), cols)]
            k = 16 + 4 * o + q
            return to_partner(ref, ref, s_p.at[part, k], r_p.at[part, k])

        def hand(o, q):
            passing(r, o, q).start()

        return Spread(at, *axes, s_p.at[part], r_p.at[part], hand), passing

    spreads, passings = zip(*(spread_of(part) for part in (0, 1)))
    together(spreads, "begin")
    send_sums(0, "tensor", z, jnp.sum((value * value).reshape(PIECE // 8, 8, RANK), axis=0))
    left[r] = left_rows(full[y, x].reshape(ROWS, RANK))
    share_left = to_partner(left.at[r], left.at[r], bs.at[1], br.at[1])
    share_left.start()
    for at_step, (job, o) in enumerate(SPREAD_STEPS):
        together(spreads, job, o)
        if at_step == 1:
            send_sums(1, "fsdp_1", x, take_sums(0, "tensor", z))
        elif at_step == 3:
            send_sums(2, "fsdp_0", y, take_sums(1, "fsdp_1", x))
        elif at_step == 5:
            norms[r] = take_sums(2, "fsdp_0", y)
            to_partner(norms.at[r], norms.at[r], bs.at[2], br.at[2]).start()
    for o in (0, 3, 1, 2):
        together(spreads, "last", o)
    together(spreads, "drain")
    together(rings, "drain")
    together(wide, "drain")
    for phase, axis, me in ((0, "tensor", z), (1, "fsdp_1", x), (2, "fsdp_0", y)):
        for k in (1, 2, 3):
            sum_copy(phase, axis, k, me).wait_send()
    for k, out in enumerate((blended, left, norms)):
        to_partner(out.at[r], out.at[r], bs.at[k], br.at[k]).wait_send()
        to_partner(out.at[other], out.at[other], bs.at[k], br.at[k]).wait_recv()
    for passing in passings:
        for o in range(4):
            for q in range(4):
                passing(r, o, q).wait_send()
                passing(other, o, q).wait_recv()


def output_kernel(left, back, blended, norms, momentum_new, update, basis_new, mom_v, up_v, base_v, sems):
    wide = COLS // CHUNKS
    dims = (((1,), (1,)), ((), ()))
    scale = math.sqrt(FEATURES * UNITS / RANK)

    def copies(i):
        w, start = i // CHUNKS, pl.multiple_of(lax.rem(i, CHUNKS) * wide, wide)
        part = pl.ds(start, wide)
        return (
            pltpu.make_async_copy(base_v.at[w, part, :], basis_new.at[w, part, :], sems.at[0, i]),
            pltpu.make_async_copy(mom_v.at[w, :, part], momentum_new.at[w, :, part], sems.at[1, i]),
            pltpu.make_async_copy(up_v.at[w, :, part], update.at[w, :, part], sems.at[2, i]),
        )

    def chunk(i, carry):
        w, start = i // CHUNKS, pl.multiple_of(lax.rem(i, CHUNKS) * wide, wide)
        part = pl.ds(start, wide)
        base, mom, up = copies(i)
        inverse = 1.0 / (jnp.sqrt(jnp.sum(norms[w], axis=0, keepdims=True)) + 1e-06)
        rows, basis = back[w, part, :], left[w]
        normed = (rows.astype(F32) * inverse).astype(BF16)
        base_v[w, part, :] = normed
        base.start()
        feedback = lax.dot_general(basis, rows, dims, preferred_element_type=F32)
        value = blended[w, :, part].astype(F32) - (1.0 - momentum_decay) * feedback
        mom_v[w, :, part] = value.astype(BF16)
        mom.start()
        value = scale * lax.dot_general(basis, normed, dims, preferred_element_type=F32)
        up_v[w, :, part] = value.astype(BF16)
        up.start()
        return carry

    lax.fori_loop(0, 2 * CHUNKS, chunk, 0)

    def finish(i, carry):
        for copy in copies(i):
            copy.wait()
        return carry

    lax.fori_loop(0, 2 * CHUNKS, finish, 0)


def shape(dims, dtype=BF16):
    return jax.ShapeDtypeStruct(dims, dtype)


VM = pl.BlockSpec(memory_space=pltpu.VMEM)
HBM = pl.BlockSpec(memory_space=pltpu.HBM)
DMA = pltpu.SemaphoreType.DMA


def shards(grads, momentum, basis):
    steps = COLS // STEP
    blended, gathered, norms, left = pl.pallas_call(
        step_kernel,
        out_shape=(
            shape((2, ROWS, COLS)),
            shape((2, 4, 4, PIECE, RANK)),
            shape((2, 8, RANK), F32),
            shape((2, ROWS, RANK)),
        ),
        in_specs=[HBM] * 3,
        out_specs=(VM,) * 4,
        scratch_shapes=[
            pltpu.VMEM((ROWS, COLS), BF16),
            pltpu.VMEM((ROWS, COLS), BF16),
            pltpu.VMEM((ROWS, COLS), BF16),
            pltpu.VMEM((COLS, RANK), BF16),
            pltpu.VMEM((ROWS, RANK), F32),
            pltpu.VMEM((COLS, ROWS), BF16),
            pltpu.VMEM((3, SLICE, RANK), BF16),
            pltpu.VMEM((3, SLICE, RANK), BF16),
            pltpu.VMEM((4, 4, 4, SLICE, RANK), BF16),
            pltpu.VMEM((4, 4, PIECE, ROWS), BF16),
            pltpu.VMEM((RANK, RANK), F32),
            pltpu.VMEM((RANK, RANK), F32),
            pltpu.VMEM((BLOCK, 2 * BLOCK), F32),
            pltpu.VMEM((BLOCK, BLOCK), F32),
            pltpu.VMEM((PIECE, RANK), F32),
            pltpu.VMEM((3, 4, 8, RANK), F32),
            DMA((3, steps)),
            DMA((steps,)),
            DMA((steps,)),
            DMA((3,)),
            DMA((3,)),
            DMA((3, 2, 16)),
            DMA((3, 2, 16)),
            DMA((16,)),
            DMA((16,)),
            DMA((3,)),
            DMA((3,)),
            DMA((3, 3)),
            DMA((3, 3)),
            DMA((2, 32)),
            DMA((2, 32)),
        ],
        compiler_params=pltpu.CompilerParams(has_side_effects=True, vmem_limit_bytes=51 << 20),
        name="step",
    )(grads, momentum, basis)
    return pl.pallas_call(
        output_kernel,
        out_shape=(shape((2, ROWS, COLS)), shape((2, ROWS, COLS)), shape((2, COLS, RANK))),
        in_specs=[VM] * 4,
        out_specs=(HBM,) * 3,
        scratch_shapes=[
            pltpu.VMEM((2, ROWS, COLS), BF16),
            pltpu.VMEM((2, ROWS, COLS), BF16),
            pltpu.VMEM((2, COLS, RANK), BF16),
            DMA((3, 2 * CHUNKS)),
        ],
        compiler_params=pltpu.CompilerParams(vmem_limit_bytes=24 << 20),
        name="outputs",
    )(left, gathered.reshape(2, COLS, RANK), blended, norms)


def solution(mesh):
    torus = Mesh(
        mesh.devices.reshape(mesh.shape["replica"], 4, 4, mesh.shape["tensor"]),
        ("replica", "fsdp_0", "fsdp_1", "tensor"),
    )
    return jax.shard_map(
        shards,
        mesh=torus,
        in_specs=(
            P("replica", None, FSDP, "tensor"),
            P(None, FSDP, "tensor"),
            P(None, "tensor", None),
        ),
        out_specs=(P(None, FSDP, "tensor"), P(None, FSDP, "tensor"), P(None, "tensor", None)),
        check_vma=False,
    )
```

```python
import functools
import math

import jax
import jax.numpy as jnp
from jax import lax
from jax.experimental import pallas as pl
from jax.experimental.pallas import tpu as pltpu
from jax.sharding import Mesh
from jax.sharding import PartitionSpec as P

FEATURES = 4096
UNITS = 14336
RANK = 512
FSDP = ("fsdp_0", "fsdp_1")
MESH = pl.DeviceIdType.MESH
BF16 = jnp.bfloat16
F32 = jnp.float32
ROWS = FEATURES // 16
COLS = UNITS // 4
PIECE = COLS // 16
SLICE = ROWS // 4
STEP = 512
PANEL = 16
BLOCK = 128
CHUNKS = 4

momentum_decay = 0.95


def coords():
    return tuple(lax.axis_index(a) for a in ("replica", "fsdp_0", "fsdp_1", "tensor"))


def shifted(i, k):
    return lax.rem(i + k, 4)


class Ring:
    def __init__(self, axis, at, send, recv):
        self.axis, self.at, self.send, self.recv = axis, at, send, recv
        me = lax.axis_index(axis)
        self.me, self.right, self.left, self.far = me, shifted(me, 1), shifted(me, 3), shifted(me, 2)

    def copy(self, k, who, half, to):
        ref = self.at(who, half)
        return pltpu.make_async_remote_copy(
            src_ref=ref,
            dst_ref=ref,
            send_sem=self.send.at[k],
            recv_sem=self.recv.at[k],
            device_id={self.axis: to},
            device_id_type=MESH,
        )

    def start(self):
        self.copy(0, self.me, None, self.right).start()
        self.copy(1, self.me, None, self.left).start()

    def middle(self):
        self.copy(0, self.left, None, self.right).wait_recv()
        self.copy(2, self.left, 0, self.right).start()
        self.copy(1, self.right, None, self.left).wait_recv()
        self.copy(3, self.right, 1, self.left).start()

    def end(self):
        self.copy(2, self.far, 0, self.right).wait_recv()
        self.copy(3, self.far, 1, self.left).wait_recv()

    def drain(self):
        self.copy(0, self.me, None, self.right).wait_send()
        self.copy(1, self.me, None, self.left).wait_send()
        self.copy(2, self.left, 0, self.right).wait_send()
        self.copy(3, self.right, 1, self.left).wait_send()


def rows_of(start, size, half):
    if half is None:
        return pl.ds(start, size)
    return pl.ds(start + half * (size // 2), size // 2)


def projected_gather(full, y, x, z, send, recv):
    parts = ((0, 32, 0, 384), (32, 32, 0, 384), (0, 64, 384, 128))

    def cut(part, half):
        r0, nr, c0, nc = parts[part]
        return rows_of(r0, nr, half), pl.ds(c0, nc)

    every = slice(None)
    plans = (
        ("tensor", "fsdp_0", "fsdp_1", lambda i: (y, x, i), lambda o, q: (shifted(y, o), shifted(x, q), every)),
        ("fsdp_1", "tensor", "fsdp_0", lambda i: (y, i, z), lambda o, q: (shifted(y, q), every, shifted(z, o))),
        ("fsdp_0", "fsdp_1", "tensor", lambda i: (i, x, z), lambda o, q: (every, shifted(x, o), shifted(z, q))),
    )
    rings, spreads = [], []
    for part, (first, line, side, ring_at, spread_at) in enumerate(plans):
        def at_ring(i, half, part=part, where=ring_at):
            return full.at[(*where(i), *cut(part, half))]

        def at_spread(o, q, half, part=part, where=spread_at):
            return full.at[(*where(o, q), *cut(part, half))]

        rings.append(Ring(first, at_ring, send.at[part, 0], recv.at[part, 0]))
        spreads.append(Spread(at_spread, line, side, send.at[part, 1], recv.at[part, 1]))
    return rings, spreads


class Spread:
    def __init__(self, at, line_axis, side_axis, send, recv, hand=None):
        self.at, self.send, self.recv = at, send, recv
        self.line_axis, self.side_axis = line_axis, side_axis
        self.hand = hand or (lambda o, q: None)
        self.sent = []

    def copy(self, k, o, q, axis, way, half=None):
        ref = self.at(o, q, half)
        return pltpu.make_async_remote_copy(
            src_ref=ref,
            dst_ref=ref,
            send_sem=self.send.at[k],
            recv_sem=self.recv.at[k],
            device_id={axis: shifted(lax.axis_index(axis), way)},
            device_id_type=MESH,
        )

    def go(self, *args):
        copy = self.copy(*args)
        copy.start()
        self.sent.append(copy)

    def begin(self):
        self.go(0, 0, 0, self.line_axis, 1)
        self.go(1, 0, 0, self.line_axis, 3)
        self.sides(0)
        self.hand(0, 0)

    def sides(self, o):
        self.go(4 + o, o, 0, self.side_axis, 1)
        self.go(8 + o, o, 0, self.side_axis, 3)

    def line(self, o):
        if o == 3:
            self.copy(0, 3, 0, self.line_axis, 1).wait_recv()
            self.go(2, 3, 0, self.line_axis, 1, 0)
        elif o == 1:
            self.copy(1, 1, 0, self.line_axis, 3).wait_recv()
            self.go(3, 1, 0, self.line_axis, 3, 1)
        else:
            self.copy(2, 2, 0, self.line_axis, 1, 0).wait_recv()
            self.copy(3, 2, 0, self.line_axis, 3, 1).wait_recv()
        self.sides(o)
        self.hand(o, 0)

    def side(self, o):
        first, second = (3, 1) if o in (0, 3) else (1, 3)
        for q in (first, second):
            if q == 3:
                self.copy(4 + o, o, 3, self.side_axis, 1).wait_recv()
            else:
                self.copy(8 + o, o, 1, self.side_axis, 3).wait_recv()
            if q == first:
                self.go(12 + o, o, q, self.side_axis, 4 - q)
            self.hand(o, q)

    def last(self, o):
        self.copy(12 + o, o, 2, self.side_axis, 1 if o in (0, 3) else 3).wait_recv()
        self.hand(o, 2)

    def drain(self):
        for copy in self.sent:
            copy.wait_send()


SPREAD_STEPS = (("line", 3), ("line", 1), ("side", 0), ("line", 2), ("side", 3), ("side", 1), ("side", 2))


def together(spreads, job, *args):
    for spread in spreads:
        getattr(spread, job)(*args)


def halves(value):
    high = value.astype(BF16)
    return high, (value - high.astype(F32)).astype(BF16)


def contract_rows(a, b):
    ah, al = halves(a)
    bh, bl = halves(b)
    return lax.dot_general(
        jnp.concatenate([ah, ah, al], axis=0),
        jnp.concatenate([bh, bl, bh], axis=0),
        (((0,), (0,)), ((), ())),
        preferred_element_type=F32,
    )


def product(a, b):
    ah, al = halves(a)
    bh, bl = halves(b)
    return jnp.dot(
        jnp.concatenate([ah, ah, al], axis=1),
        jnp.concatenate([bh, bl, bh], axis=0),
        preferred_element_type=F32,
    )


def eliminate(work, inverse):
    row = lax.broadcasted_iota(jnp.int32, (PANEL, BLOCK), 0)
    lane = lax.broadcasted_iota(jnp.int32, (BLOCK, BLOCK), 1)

    def panel(p, carry):
        left, right = work[0:PANEL, 0:BLOCK], work[0:PANEL, BLOCK:]
        columns = [jnp.broadcast_to(left[:, k : k + 1], (PANEL, BLOCK)) for k in range(PANEL)]
        inverses = jnp.ones((PANEL, BLOCK), F32)
        for j in range(PANEL):
            inv = 1.0 / columns[j][j : j + 1, :]
            times = jnp.where(row > j, columns[j] * inv, 0.0)
            for k in range(j + 1, PANEL):
                columns[k] = columns[k] - times * columns[k][j : j + 1, :]
            left = left - times * left[j : j + 1, :]
            right = right - times * right[j : j + 1, :]
            inverses = jnp.where(row == j, inv, inverses)
        scale = jnp.sqrt(inverses)
        left, right = left * scale, right * scale
        inverse[pl.ds(pl.multiple_of(p * PANEL, PANEL), PANEL), :] = right
        change = contract_rows(left, jnp.concatenate([left, right], axis=1))
        rest = work[:, 0:BLOCK] - change[:, 0:BLOCK]
        rest = jnp.where(lane < BLOCK - PANEL, pltpu.roll(rest, BLOCK - PANEL, 1), 0.0)
        work[0 : BLOCK - PANEL, 0:BLOCK] = rest[PANEL:, :]
        extra = work[:, BLOCK:] - change[:, BLOCK:]
        work[0 : BLOCK - PANEL, BLOCK:] = extra[PANEL:, :]
        work[BLOCK - PANEL :, :] = jnp.zeros((PANEL, 2 * BLOCK), F32)
        return carry

    lax.fori_loop(0, BLOCK // PANEL, panel, 0)


def factor_inverse(gram, low, work, inverse):
    low[...] = jnp.zeros_like(low)
    count = RANK // BLOCK
    square = (BLOCK, BLOCK)
    eye = jnp.where(
        lax.broadcasted_iota(jnp.int32, square, 0) == lax.broadcasted_iota(jnp.int32, square, 1), 1.0, 0.0
    )
    for k in range(count):
        here, after = slice(k * BLOCK, (k + 1) * BLOCK), slice((k + 1) * BLOCK, RANK)
        work[:, 0:BLOCK] = gram[here, here]
        work[:, BLOCK:] = eye
        eliminate(work, inverse)
        block = inverse[...]
        if k:
            low[here, 0 : k * BLOCK] = product(block, low[here, 0 : k * BLOCK])
        low[here, here] = block
        if k < count - 1:
            upper = product(block, gram[here, after])
            gram[after, after] = gram[after, after] - contract_rows(upper, upper)
            done = slice(0, (k + 1) * BLOCK)
            low[after, done] = low[after, done] - contract_rows(upper, low[here, done])


def meet(y, x, z, other):
    barrier = pltpu.get_barrier_semaphore()
    peers = [{"replica": other}] + [{"tensor": shifted(z, k)} for k in (1, 2, 3)]
    peers += [{"fsdp_0": shifted(y, k // 4), "fsdp_1": shifted(x, k % 4)} for k in range(1, 16)]
    for peer in peers:
        pl.semaphore_signal(barrier, inc=1, device_id=peer, device_id_type=MESH)
    pl.semaphore_wait(barrier, len(peers))


def step_kernel(
    grads, momentum, basis, blended, blended_too, gathered, gathered_too, norms, left,
    m_v, g_v, gp_v, b_v, acc, flipped, out_z, in_z, full, turned, gram, low, work, inverse, total, sums,
    load, gs, gr, zs, zr, ags, agr, ts, tr, bs, br, s_n, r_n, s_p, r_p,
):
    r, y, x, z = coords()
    other = 1 - r
    steps = COLS // STEP

    def grad_copy(c, cols):
        return pltpu.make_async_remote_copy(
            src_ref=grads.at[0, other, :, cols],
            dst_ref=gp_v.at[:, cols],
            send_sem=gs.at[c],
            recv_sem=gr.at[c],
            device_id={"replica": other},
            device_id_type=MESH,
        )

    def loads(c, cols):
        return (
            pltpu.make_async_copy(grads.at[0, r, :, cols], g_v.at[:, cols], load.at[0, c]),
            pltpu.make_async_copy(momentum.at[r, :, cols], m_v.at[:, cols], load.at[1, c]),
            pltpu.make_async_copy(basis.at[r, cols, :], b_v.at[cols, :], load.at[2, c]),
        )

    for c in range(steps):
        for copy in loads(c, pl.ds(c * STEP, STEP)):
            copy.start()
    meet(y, x, z, other)
    for c in range(steps):
        grad_copy(c, pl.ds(c * STEP, STEP)).start()
    acc[...] = jnp.zeros_like(acc)

    def blend(c, carry):
        cols = pl.ds(pl.multiple_of(c * STEP, STEP), STEP)
        for copy in loads(c, cols):
            copy.wait()
        grad_copy(c, cols).wait()
        both = g_v[:, cols].astype(F32) + gp_v[:, cols].astype(F32)
        value = (m_v[:, cols].astype(F32) + both).astype(BF16)
        blended[:, cols] = value
        acc[...] += jnp.dot(value, b_v[cols, :], preferred_element_type=F32)
        return carry

    lax.fori_loop(0, steps, blend, 0)

    def z_copy(k):
        return pltpu.make_async_remote_copy(
            src_ref=out_z.at[k - 1],
            dst_ref=in_z.at[k - 1],
            send_sem=zs.at[k - 1],
            recv_sem=zr.at[k - 1],
            device_id={"tensor": shifted(z, k)},
            device_id_type=MESH,
        )

    for k in (2, 1, 3):
        rows = pl.ds(pl.multiple_of(shifted(z, k) * SLICE, SLICE), SLICE)
        out_z[k - 1] = acc[rows, :].astype(BF16)
        z_copy(k).start()

    def flip(c, carry):
        cols = pl.ds(pl.multiple_of(c * STEP, STEP), STEP)
        flipped[cols, :] = blended[:, cols].T
        return carry

    lax.fori_loop(0, steps, flip, 0)
    piece = acc[pl.ds(pl.multiple_of(z * SLICE, SLICE), SLICE), :]
    for k in (1, 3, 2):
        z_copy(k).wait()
        piece = piece + in_z[k - 1].astype(F32)
    full[y, x, z] = piece.astype(BF16)

    rings, wide = projected_gather(full, y, x, z, ags, agr)
    together(rings, "start")
    together(rings, "middle")
    together(rings, "end")
    together(wide, "begin")
    for job, o in SPREAD_STEPS:
        together(wide, job, o)

    def turn_copy(k):
        ty, tx = shifted(y, k // 4), shifted(x, k % 4)
        start = pl.multiple_of((ty * 4 + tx) * PIECE, PIECE)
        return pltpu.make_async_remote_copy(
            src_ref=flipped.at[pl.ds(start, PIECE), :],
            dst_ref=turned.at[y, x],
            send_sem=ts.at[k],
            recv_sem=tr.at[k],
            device_id={"fsdp_0": ty, "fsdp_1": tx},
            device_id_type=MESH,
        )

    def turn_arrival(k):
        sy, sx = shifted(y, 4 - k // 4), shifted(x, 4 - k % 4)
        return pltpu.make_async_remote_copy(
            src_ref=turned.at[sy, sx],
            dst_ref=turned.at[sy, sx],
            send_sem=ts.at[k],
            recv_sem=tr.at[k],
            device_id={"fsdp_0": sy, "fsdp_1": sx},
            device_id_type=MESH,
        )

    for k in range(1, 16):
        turn_copy(k).start()

    def to_partner(src, dst, send, recv):
        return pltpu.make_async_remote_copy(
            src_ref=src,
            dst_ref=dst,
            send_sem=send,
            recv_sem=recv,
            device_id={"replica": other},
            device_id_type=MESH,
        )

    share = to_partner(blended, blended_too, bs.at[0], br.at[0])
    share.start()
    turned[y, x] = flipped[pl.ds(pl.multiple_of((y * 4 + x) * PIECE, PIECE), PIECE), :]
    for o in (0, 3, 1, 2):
        together(wide, "last", o)

    gram[...] = jnp.zeros_like(gram)

    def add_gram(b, carry):
        rows = full[b].reshape(4 * ROWS, RANK)
        gram[...] += lax.dot_general(rows, rows, (((0,), (0,)), ((), ())), preferred_element_type=F32)
        return carry

    lax.fori_loop(0, 4, add_gram, 0)
    factor_inverse(gram, low, work, inverse)
    high = low[...].astype(BF16)
    total[...] = jnp.zeros_like(total)
    dims = (((1,), (1,)), ((), ()))

    def left_rows(rows):
        return lax.dot_general(rows, high, dims, preferred_element_type=F32).astype(BF16)

    for k in range(1, 16):
        turn_copy(k).wait_send()
        turn_arrival(k).wait_recv()

    def add_back(b, carry):
        rows = left_rows(full[b].reshape(4 * ROWS, RANK))
        for bx in range(4):
            total[...] += jnp.dot(turned[b, bx], rows[bx * ROWS : (bx + 1) * ROWS], preferred_element_type=F32)
        return carry

    lax.fori_loop(0, 4, add_back, 0)
    value = total[...]
    gathered[y, x] = value.astype(BF16)

    def sum_copy(phase, axis, k, me):
        return pltpu.make_async_remote_copy(
            src_ref=sums.at[phase, me],
            dst_ref=sums.at[phase, me],
            send_sem=s_n.at[phase, k - 1],
            recv_sem=r_n.at[phase, k - 1],
            device_id={axis: shifted(me, k)},
            device_id_type=MESH,
        )

    def sum_arrival(phase, axis, k, me):
        source = shifted(me, 4 - k)
        return pltpu.make_async_remote_copy(
            src_ref=sums.at[phase, source],
            dst_ref=sums.at[phase, source],
            send_sem=s_n.at[phase, k - 1],
            recv_sem=r_n.at[phase, k - 1],
            device_id={axis: source},
            device_id_type=MESH,
        )

    def send_sums(phase, axis, me, block):
        sums[phase, me] = block
        for k in (2, 1, 3):
            sum_copy(phase, axis, k, me).start()

    def take_sums(phase, axis, me):
        for k in (1, 3, 2):
            sum_arrival(phase, axis, k, me).wait_recv()
        return (sums[phase, 0] + sums[phase, 1]) + (sums[phase, 2] + sums[phase, 3])

    def spread_of(part):
        cols = pl.ds(part * (RANK // 2), RANK // 2)
        axes = ("fsdp_0", "fsdp_1") if part == 0 else ("fsdp_1", "fsdp_0")

        def place(o, q):
            return (shifted(y, o), shifted(x, q)) if part == 0 else (shifted(y, q), shifted(x, o))

        def at(o, q, half):
            return gathered.at[(*place(o, q), rows_of(0, PIECE, half), cols)]

        def passing(o, q):
            where = (*place(o, q), slice(None), cols)
            k = 16 + 4 * o + q
            return to_partner(gathered.at[where], gathered_too.at[where], s_p.at[part, k], r_p.at[part, k])

        def hand(o, q):
            passing(o, q).start()

        return Spread(at, *axes, s_p.at[part], r_p.at[part], hand), passing

    spreads, passings = zip(*(spread_of(part) for part in (0, 1)))
    together(spreads, "begin")
    send_sums(0, "tensor", z, jnp.sum((value * value).reshape(PIECE // 8, 8, RANK), axis=0))
    left[0] = left_rows(full[y, x].reshape(ROWS, RANK))
    share_left = to_partner(left.at[0], left.at[1], bs.at[1], br.at[1])
    share_left.start()
    for at_step, (job, o) in enumerate(SPREAD_STEPS):
        together(spreads, job, o)
        if at_step == 1:
            send_sums(1, "fsdp_1", x, take_sums(0, "tensor", z))
        elif at_step == 3:
            send_sums(2, "fsdp_0", y, take_sums(1, "fsdp_1", x))
        elif at_step == 5:
            norms[0] = take_sums(2, "fsdp_0", y)
            share_norms = to_partner(norms.at[0], norms.at[1], bs.at[2], br.at[2])
            share_norms.start()
    for o in (0, 3, 1, 2):
        together(spreads, "last", o)
    together(spreads, "drain")
    together(rings, "drain")
    together(wide, "drain")
    for phase, axis, me in ((0, "tensor", z), (1, "fsdp_1", x), (2, "fsdp_0", y)):
        for k in (1, 2, 3):
            sum_copy(phase, axis, k, me).wait_send()
    share.wait()
    share_left.wait()
    share_norms.wait()
    for passing in passings:
        for o in range(4):
            for q in range(4):
                passing(o, q).wait()


def output_kernel(left, back, back_too, blended, blended_too, norms, momentum_new, update, basis_new, mom_v, up_v, base_v, sems):
    wide = COLS // CHUNKS
    dims = (((1,), (1,)), ((), ()))
    scale = math.sqrt(FEATURES * UNITS / RANK)
    me = lax.axis_index("replica")

    def copies(half, i):
        part = pl.ds(pl.multiple_of(i * wide, wide), wide)
        w = me if half == 0 else 1 - me
        return part, (
            pltpu.make_async_copy(base_v.at[half, part, :], basis_new.at[w, part, :], sems.at[0, half, i]),
            pltpu.make_async_copy(mom_v.at[half, :, part], momentum_new.at[w, :, part], sems.at[1, half, i]),
            pltpu.make_async_copy(up_v.at[half, :, part], update.at[w, :, part], sems.at[2, half, i]),
        )

    for half, (rows_ref, old) in enumerate(((back, blended), (back_too, blended_too))):
        inverse = 1.0 / (jnp.sqrt(jnp.sum(norms[half], axis=0, keepdims=True)) + 1e-06)
        basis = left[half]

        def chunk(i, carry, half=half, rows_ref=rows_ref, old=old, inverse=inverse, basis=basis):
            part, (base, mom, up) = copies(half, i)
            rows = rows_ref[part, :]
            normed = (rows.astype(F32) * inverse).astype(BF16)
            base_v[half, part, :] = normed
            base.start()
            feedback = lax.dot_general(basis, rows, dims, preferred_element_type=F32)
            value = old[:, part].astype(F32) - (1.0 - momentum_decay) * feedback
            mom_v[half, :, part] = value.astype(BF16)
            mom.start()
            value = scale * lax.dot_general(basis, normed, dims, preferred_element_type=F32)
            up_v[half, :, part] = value.astype(BF16)
            up.start()
            return carry

        lax.fori_loop(0, CHUNKS, chunk, 0)
    for half in range(2):

        def finish(i, carry, half=half):
            for copy in copies(half, i)[1]:
                copy.wait()
            return carry

        lax.fori_loop(0, CHUNKS, finish, 0)


def shape(dims, dtype=BF16):
    return jax.ShapeDtypeStruct(dims, dtype)


VM = pl.BlockSpec(memory_space=pltpu.VMEM)
HBM = pl.BlockSpec(memory_space=pltpu.HBM)
DMA = pltpu.SemaphoreType.DMA


def shards(grads, momentum, basis):
    steps = COLS // STEP
    blended, blended_too, gathered, gathered_too, norms, left = pl.pallas_call(
        step_kernel,
        out_shape=(
            shape((ROWS, COLS)),
            shape((ROWS, COLS)),
            shape((4, 4, PIECE, RANK)),
            shape((4, 4, PIECE, RANK)),
            shape((2, 8, RANK), F32),
            shape((2, ROWS, RANK)),
        ),
        in_specs=[HBM] * 3,
        out_specs=(VM,) * 6,
        scratch_shapes=[
            pltpu.VMEM((ROWS, COLS), BF16),
            pltpu.VMEM((ROWS, COLS), BF16),
            pltpu.VMEM((ROWS, COLS), BF16),
            pltpu.VMEM((COLS, RANK), BF16),
            pltpu.VMEM((ROWS, RANK), F32),
            pltpu.VMEM((COLS, ROWS), BF16),
            pltpu.VMEM((3, SLICE, RANK), BF16),
            pltpu.VMEM((3, SLICE, RANK), BF16),
            pltpu.VMEM((4, 4, 4, SLICE, RANK), BF16),
            pltpu.VMEM((4, 4, PIECE, ROWS), BF16),
            pltpu.VMEM((RANK, RANK), F32),
            pltpu.VMEM((RANK, RANK), F32),
            pltpu.VMEM((BLOCK, 2 * BLOCK), F32),
            pltpu.VMEM((BLOCK, BLOCK), F32),
            pltpu.VMEM((PIECE, RANK), F32),
            pltpu.VMEM((3, 4, 8, RANK), F32),
            DMA((3, steps)),
            DMA((steps,)),
            DMA((steps,)),
            DMA((3,)),
            DMA((3,)),
            DMA((3, 2, 16)),
            DMA((3, 2, 16)),
            DMA((16,)),
            DMA((16,)),
            DMA((3,)),
            DMA((3,)),
            DMA((3, 3)),
            DMA((3, 3)),
            DMA((2, 32)),
            DMA((2, 32)),
        ],
        compiler_params=pltpu.CompilerParams(collective_id=0, has_side_effects=True, vmem_limit_bytes=42 << 20),
        name="step",
    )(grads, momentum, basis)
    return pl.pallas_call(
        output_kernel,
        out_shape=(shape((2, ROWS, COLS)), shape((2, ROWS, COLS)), shape((2, COLS, RANK))),
        in_specs=[VM] * 6,
        out_specs=(HBM,) * 3,
        scratch_shapes=[
            pltpu.VMEM((2, ROWS, COLS), BF16),
            pltpu.VMEM((2, ROWS, COLS), BF16),
            pltpu.VMEM((2, COLS, RANK), BF16),
            DMA((3, 2, CHUNKS)),
        ],
        compiler_params=pltpu.CompilerParams(vmem_limit_bytes=24 << 20),
        name="outputs",
    )(left, gathered.reshape(COLS, RANK), gathered_too.reshape(COLS, RANK), blended, blended_too, norms)


def solution(mesh):
    torus = Mesh(
        mesh.devices.reshape(mesh.shape["replica"], 4, 4, mesh.shape["tensor"]),
        ("replica", "fsdp_0", "fsdp_1", "tensor"),
    )
    return jax.shard_map(
        shards,
        mesh=torus,
        in_specs=(
            P("replica", None, FSDP, "tensor"),
            P(None, FSDP, "tensor"),
            P(None, "tensor", None),
        ),
        out_specs=(P(None, FSDP, "tensor"), P(None, FSDP, "tensor"), P(None, "tensor", None)),
        check_vma=False,
    )
```

```python
import functools
import math

import jax
import jax.numpy as jnp
from jax import lax
from jax.experimental import pallas as pl
from jax.experimental.pallas import tpu as pltpu
from jax.sharding import Mesh
from jax.sharding import PartitionSpec as P

FEATURES = 4096
UNITS = 14336
RANK = 512
FSDP = ("fsdp_0", "fsdp_1")
MESH = pl.DeviceIdType.MESH
BF16 = jnp.bfloat16
F32 = jnp.float32
ROWS = FEATURES // 16
COLS = UNITS // 4
PIECE = COLS // 16
SLICE = ROWS // 4
STEP = 512
PANEL = 16
BLOCK = 128
CHUNKS = 4

momentum_decay = 0.95


def coords():
    return tuple(lax.axis_index(a) for a in ("replica", "fsdp_0", "fsdp_1", "tensor"))


def shifted(i, k):
    return lax.rem(i + k, 4)


class Ring:
    def __init__(self, axis, at, send, recv):
        self.axis, self.at, self.send, self.recv = axis, at, send, recv

    def copy(self, k, arriving):
        me = lax.axis_index(self.axis)
        ref = self.at(shifted(me, 4 - k) if arriving else me)
        return pltpu.make_async_remote_copy(
            src_ref=ref,
            dst_ref=ref,
            send_sem=self.send.at[k],
            recv_sem=self.recv.at[k],
            device_id={self.axis: shifted(me, k)},
            device_id_type=MESH,
        )

    def start(self):
        for k in (2, 1, 3):
            self.copy(k, False).start()

    def end(self):
        for k in (1, 3, 2):
            self.copy(k, True).wait_recv()

    def drain(self):
        for k in (1, 2, 3):
            self.copy(k, False).wait_send()


def rows_of(start, size, half):
    if half is None:
        return pl.ds(start, size)
    return pl.ds(start + half * (size // 2), size // 2)


def projected_gather(full, y, x, z, send, recv):
    parts = ((0, 32, 0, 384), (32, 32, 0, 384), (0, 64, 384, 128))

    def cut(part, half):
        r0, nr, c0, nc = parts[part]
        return rows_of(r0, nr, half), pl.ds(c0, nc)

    every = slice(None)
    plans = (
        ("tensor", "fsdp_0", "fsdp_1", lambda i: (y, x, i), lambda o, q: (shifted(y, o), shifted(x, q), every)),
        ("fsdp_1", "tensor", "fsdp_0", lambda i: (y, i, z), lambda o, q: (shifted(y, q), every, shifted(z, o))),
        ("fsdp_0", "fsdp_1", "tensor", lambda i: (i, x, z), lambda o, q: (every, shifted(x, o), shifted(z, q))),
    )
    rings, spreads = [], []
    for part, (first, line, side, ring_at, spread_at) in enumerate(plans):
        def at_ring(i, part=part, where=ring_at):
            return full.at[(*where(i), *cut(part, None))]

        def at_spread(o, q, half, part=part, where=spread_at):
            return full.at[(*where(o, q), *cut(part, half))]

        rings.append(Ring(first, at_ring, send.at[part, 0], recv.at[part, 0]))
        spreads.append(Spread(at_spread, line, side, send.at[part, 1], recv.at[part, 1]))
    return rings, spreads


class Spread:
    def __init__(self, at, line_axis, side_axis, send, recv, hand=None):
        self.at, self.send, self.recv = at, send, recv
        self.line_axis, self.side_axis = line_axis, side_axis
        self.hand = hand or (lambda o, q: None)
        self.sent = []

    def copy(self, k, o, q, axis, way, half=None):
        ref = self.at(o, q, half)
        return pltpu.make_async_remote_copy(
            src_ref=ref,
            dst_ref=ref,
            send_sem=self.send.at[k],
            recv_sem=self.recv.at[k],
            device_id={axis: shifted(lax.axis_index(axis), way)},
            device_id_type=MESH,
        )

    def go(self, *args):
        copy = self.copy(*args)
        copy.start()
        self.sent.append(copy)

    def begin(self):
        self.go(0, 0, 0, self.line_axis, 1)
        self.go(1, 0, 0, self.line_axis, 3)
        self.sides(0)
        self.hand(0, 0)

    def sides(self, o):
        self.go(4 + o, o, 0, self.side_axis, 1)
        self.go(8 + o, o, 0, self.side_axis, 3)

    def line(self, o):
        if o == 3:
            self.copy(0, 3, 0, self.line_axis, 1).wait_recv()
            self.go(2, 3, 0, self.line_axis, 1, 0)
        elif o == 1:
            self.copy(1, 1, 0, self.line_axis, 3).wait_recv()
            self.go(3, 1, 0, self.line_axis, 3, 1)
        else:
            self.copy(2, 2, 0, self.line_axis, 1, 0).wait_recv()
            self.copy(3, 2, 0, self.line_axis, 3, 1).wait_recv()
        self.sides(o)
        self.hand(o, 0)

    def side(self, o):
        first, second = (3, 1) if o in (0, 3) else (1, 3)
        for q in (first, second):
            if q == 3:
                self.copy(4 + o, o, 3, self.side_axis, 1).wait_recv()
            else:
                self.copy(8 + o, o, 1, self.side_axis, 3).wait_recv()
            if q == first:
                self.go(12 + o, o, q, self.side_axis, 4 - q)
            self.hand(o, q)

    def last(self, o):
        self.copy(12 + o, o, 2, self.side_axis, 1 if o in (0, 3) else 3).wait_recv()
        self.hand(o, 2)

    def drain(self):
        for copy in self.sent:
            copy.wait_send()


SPREAD_STEPS = (("line", 3), ("line", 1), ("side", 0), ("line", 2), ("side", 3), ("side", 1), ("side", 2))


def together(spreads, job, *args):
    for spread in spreads:
        getattr(spread, job)(*args)


def halves(value):
    high = value.astype(BF16)
    return high, (value - high.astype(F32)).astype(BF16)


def contract_rows(a, b):
    ah, al = halves(a)
    bh, bl = halves(b)
    return lax.dot_general(
        jnp.concatenate([ah, ah, al], axis=0),
        jnp.concatenate([bh, bl, bh], axis=0),
        (((0,), (0,)), ((), ())),
        preferred_element_type=F32,
    )


def product(a, b):
    ah, al = halves(a)
    bh, bl = halves(b)
    return jnp.dot(
        jnp.concatenate([ah, ah, al], axis=1),
        jnp.concatenate([bh, bl, bh], axis=0),
        preferred_element_type=F32,
    )


def times_transpose(a, b):
    ah, al = halves(a)
    bh, bl = halves(b)
    return lax.dot_general(
        jnp.concatenate([ah, ah, al], axis=1),
        jnp.concatenate([bh, bl, bh], axis=1),
        (((1,), (1,)), ((), ())),
        preferred_element_type=F32,
    )


def eliminate(work, inverse):
    row = lax.broadcasted_iota(jnp.int32, (PANEL, BLOCK), 0)
    lane = lax.broadcasted_iota(jnp.int32, (BLOCK, BLOCK), 1)

    def panel(p, carry):
        left, right = work[0:PANEL, 0:BLOCK], work[0:PANEL, BLOCK:]
        columns = [jnp.broadcast_to(left[:, k : k + 1], (PANEL, BLOCK)) for k in range(PANEL)]
        inverses = jnp.ones((PANEL, BLOCK), F32)
        for j in range(PANEL):
            inv = 1.0 / columns[j][j : j + 1, :]
            times = jnp.where(row > j, columns[j] * inv, 0.0)
            for k in range(j + 1, PANEL):
                columns[k] = columns[k] - times * columns[k][j : j + 1, :]
            left = left - times * left[j : j + 1, :]
            right = right - times * right[j : j + 1, :]
            inverses = jnp.where(row == j, inv, inverses)
        scale = jnp.sqrt(inverses)
        left, right = left * scale, right * scale
        inverse[pl.ds(pl.multiple_of(p * PANEL, PANEL), PANEL), :] = right
        change = contract_rows(left, jnp.concatenate([left, right], axis=1))
        rest = work[:, 0:BLOCK] - change[:, 0:BLOCK]
        rest = jnp.where(lane < BLOCK - PANEL, pltpu.roll(rest, BLOCK - PANEL, 1), 0.0)
        work[0 : BLOCK - PANEL, 0:BLOCK] = rest[PANEL:, :]
        extra = work[:, BLOCK:] - change[:, BLOCK:]
        work[0 : BLOCK - PANEL, BLOCK:] = extra[PANEL:, :]
        work[BLOCK - PANEL :, :] = jnp.zeros((PANEL, 2 * BLOCK), F32)
        return carry

    lax.fori_loop(0, BLOCK // PANEL, panel, 0)


def factor_inverse(gram, low, work, inverse):
    low[...] = jnp.zeros_like(low)
    count = RANK // BLOCK
    square = (BLOCK, BLOCK)
    eye = jnp.where(
        lax.broadcasted_iota(jnp.int32, square, 0) == lax.broadcasted_iota(jnp.int32, square, 1), 1.0, 0.0
    )
    for k in range(count):
        here, after = slice(k * BLOCK, (k + 1) * BLOCK), slice((k + 1) * BLOCK, RANK)
        work[:, 0:BLOCK] = gram[here, here]
        work[:, BLOCK:] = eye
        eliminate(work, inverse)
        block = inverse[...]
        if k:
            low[here, 0 : k * BLOCK] = product(block, low[here, 0 : k * BLOCK])
        low[here, here] = block
        if k < count - 1:
            upper = product(block, gram[here, after])
            gram[after, after] = gram[after, after] - contract_rows(upper, upper)
            done = slice(0, (k + 1) * BLOCK)
            low[after, done] = low[after, done] - contract_rows(upper, low[here, done])


NEAR = (1, 3, 4, 12)


def meet(y, x, z, other):
    barrier = pltpu.get_barrier_semaphore()
    peers = [{"replica": other}] + [{"tensor": shifted(z, k)} for k in (1, 2, 3)]
    peers += [{"fsdp_0": shifted(y, k // 4), "fsdp_1": shifted(x, k % 4)} for k in range(1, 16)]
    for peer in peers:
        pl.semaphore_signal(barrier, inc=1, device_id=peer, device_id_type=MESH)
    pl.semaphore_wait(barrier, len(peers))


def step_kernel(
    grads, momentum, basis, blended, blended_too, gathered, gathered_too, norms, left,
    m_v, g_v, gp_v, b_v, acc, flipped, out_z, in_z, full, turned, gram, low, work, inverse, total, sums,
    load, gs, gr, zs, zr, ags, agr, ts, tr, bs, br, s_n, r_n, s_p, r_p,
):
    r, y, x, z = coords()
    other = 1 - r
    steps = COLS // STEP

    def grad_copy(c, cols):
        return pltpu.make_async_remote_copy(
            src_ref=grads.at[0, other, :, cols],
            dst_ref=gp_v.at[:, cols],
            send_sem=gs.at[c],
            recv_sem=gr.at[c],
            device_id={"replica": other},
            device_id_type=MESH,
        )

    def loads(c, cols):
        return (
            pltpu.make_async_copy(grads.at[0, r, :, cols], g_v.at[:, cols], load.at[0, c]),
            pltpu.make_async_copy(momentum.at[r, :, cols], m_v.at[:, cols], load.at[1, c]),
            pltpu.make_async_copy(basis.at[r, cols, :], b_v.at[cols, :], load.at[2, c]),
        )

    for c in range(steps):
        for copy in loads(c, pl.ds(c * STEP, STEP)):
            copy.start()
    meet(y, x, z, other)
    for c in range(steps):
        grad_copy(c, pl.ds(c * STEP, STEP)).start()
    acc[...] = jnp.zeros_like(acc)

    def blend(c, carry):
        cols = pl.ds(pl.multiple_of(c * STEP, STEP), STEP)
        for copy in loads(c, cols):
            copy.wait()
        grad_copy(c, cols).wait()
        both = g_v[:, cols].astype(F32) + gp_v[:, cols].astype(F32)
        value = (m_v[:, cols].astype(F32) + both).astype(BF16)
        blended[:, cols] = value
        acc[...] += jnp.dot(value, b_v[cols, :], preferred_element_type=F32)
        return carry

    lax.fori_loop(0, steps, blend, 0)

    def z_copy(k):
        return pltpu.make_async_remote_copy(
            src_ref=out_z.at[k - 1],
            dst_ref=in_z.at[k - 1],
            send_sem=zs.at[k - 1],
            recv_sem=zr.at[k - 1],
            device_id={"tensor": shifted(z, k)},
            device_id_type=MESH,
        )

    for k in (2, 1, 3):
        rows = pl.ds(pl.multiple_of(shifted(z, k) * SLICE, SLICE), SLICE)
        out_z[k - 1] = acc[rows, :].astype(BF16)
        z_copy(k).start()

    def flip(c, carry):
        cols = pl.ds(pl.multiple_of(c * STEP, STEP), STEP)
        flipped[cols, :] = blended[:, cols].T
        return carry

    lax.fori_loop(0, steps, flip, 0)
    def turn_copy(k):
        ty, tx = shifted(y, k // 4), shifted(x, k % 4)
        start = pl.multiple_of((ty * 4 + tx) * PIECE, PIECE)
        return pltpu.make_async_remote_copy(
            src_ref=flipped.at[pl.ds(start, PIECE), :],
            dst_ref=turned.at[y, x],
            send_sem=ts.at[k],
            recv_sem=tr.at[k],
            device_id={"fsdp_0": ty, "fsdp_1": tx},
            device_id_type=MESH,
        )

    for k in NEAR:
        turn_copy(k).start()
    piece = acc[pl.ds(pl.multiple_of(z * SLICE, SLICE), SLICE), :]
    for k in (1, 3, 2):
        z_copy(k).wait()
        piece = piece + in_z[k - 1].astype(F32)
    full[y, x, z] = piece.astype(BF16)

    rings, wide = projected_gather(full, y, x, z, ags, agr)
    together(rings, "start")
    together(rings, "end")
    together(wide, "begin")
    for job, o in SPREAD_STEPS:
        together(wide, job, o)

    def turn_arrival(k):
        sy, sx = shifted(y, 4 - k // 4), shifted(x, 4 - k % 4)
        return pltpu.make_async_remote_copy(
            src_ref=turned.at[sy, sx],
            dst_ref=turned.at[sy, sx],
            send_sem=ts.at[k],
            recv_sem=tr.at[k],
            device_id={"fsdp_0": sy, "fsdp_1": sx},
            device_id_type=MESH,
        )

    for k in range(1, 16):
        if k not in NEAR:
            turn_copy(k).start()

    def to_partner(src, dst, send, recv):
        return pltpu.make_async_remote_copy(
            src_ref=src,
            dst_ref=dst,
            send_sem=send,
            recv_sem=recv,
            device_id={"replica": other},
            device_id_type=MESH,
        )

    share = to_partner(blended, blended_too, bs.at[0], br.at[0])
    share.start()
    turned[y, x] = flipped[pl.ds(pl.multiple_of((y * 4 + x) * PIECE, PIECE), PIECE), :]
    for o in (0, 3, 1, 2):
        together(wide, "last", o)

    gram[...] = jnp.zeros_like(gram)

    def add_gram(b, carry):
        rows = full[b].reshape(4 * ROWS, RANK)
        gram[...] += lax.dot_general(rows, rows, (((0,), (0,)), ((), ())), preferred_element_type=F32)
        return carry

    lax.fori_loop(0, 4, add_gram, 0)
    factor_inverse(gram, low, work, inverse)
    high = low[...].astype(BF16)
    total[...] = jnp.zeros_like(total)
    dims = (((1,), (1,)), ((), ()))

    def left_rows(rows):
        return lax.dot_general(rows, high, dims, preferred_element_type=F32).astype(BF16)

    for k in range(1, 16):
        turn_copy(k).wait_send()
        turn_arrival(k).wait_recv()

    def add_back(b, carry):
        rows = full[b].reshape(4 * ROWS, RANK)
        columns = jnp.concatenate([turned[b, bx] for bx in range(4)], axis=1)
        total[...] += jnp.dot(columns, rows, preferred_element_type=F32)
        return carry

    lax.fori_loop(0, 4, add_back, 0)
    value = times_transpose(total[...], low[...])
    gathered[y, x] = value.astype(BF16)

    def sum_copy(phase, axis, k, me):
        return pltpu.make_async_remote_copy(
            src_ref=sums.at[phase, me],
            dst_ref=sums.at[phase, me],
            send_sem=s_n.at[phase, k - 1],
            recv_sem=r_n.at[phase, k - 1],
            device_id={axis: shifted(me, k)},
            device_id_type=MESH,
        )

    def sum_arrival(phase, axis, k, me):
        source = shifted(me, 4 - k)
        return pltpu.make_async_remote_copy(
            src_ref=sums.at[phase, source],
            dst_ref=sums.at[phase, source],
            send_sem=s_n.at[phase, k - 1],
            recv_sem=r_n.at[phase, k - 1],
            device_id={axis: source},
            device_id_type=MESH,
        )

    def send_sums(phase, axis, me, block):
        sums[phase, me] = block
        for k in (2, 1, 3):
            sum_copy(phase, axis, k, me).start()

    def take_sums(phase, axis, me):
        for k in (1, 3, 2):
            sum_arrival(phase, axis, k, me).wait_recv()
        return (sums[phase, 0] + sums[phase, 1]) + (sums[phase, 2] + sums[phase, 3])

    def spread_of(part):
        cols = pl.ds(part * (RANK // 2), RANK // 2)
        axes = ("fsdp_0", "fsdp_1") if part == 0 else ("fsdp_1", "fsdp_0")

        def place(o, q):
            return (shifted(y, o), shifted(x, q)) if part == 0 else (shifted(y, q), shifted(x, o))

        def at(o, q, half):
            return gathered.at[(*place(o, q), rows_of(0, PIECE, half), cols)]

        def passing(o, q):
            where = (*place(o, q), slice(None), cols)
            k = 16 + 4 * o + q
            return to_partner(gathered.at[where], gathered_too.at[where], s_p.at[part, k], r_p.at[part, k])

        def hand(o, q):
            passing(o, q).start()

        return Spread(at, *axes, s_p.at[part], r_p.at[part], hand), passing

    spreads, passings = zip(*(spread_of(part) for part in (0, 1)))
    together(spreads, "begin")
    send_sums(0, "tensor", z, jnp.sum((value * value).reshape(PIECE // 8, 8, RANK), axis=0))
    left[0] = left_rows(full[y, x].reshape(ROWS, RANK))
    share_left = to_partner(left.at[0], left.at[1], bs.at[1], br.at[1])
    share_left.start()
    for at_step, (job, o) in enumerate(SPREAD_STEPS):
        together(spreads, job, o)
        if at_step == 1:
            send_sums(1, "fsdp_1", x, take_sums(0, "tensor", z))
        elif at_step == 3:
            send_sums(2, "fsdp_0", y, take_sums(1, "fsdp_1", x))
        elif at_step == 5:
            norms[0] = take_sums(2, "fsdp_0", y)
            share_norms = to_partner(norms.at[0], norms.at[1], bs.at[2], br.at[2])
            share_norms.start()
    for o in (0, 3, 1, 2):
        together(spreads, "last", o)
    together(spreads, "drain")
    together(rings, "drain")
    together(wide, "drain")
    for phase, axis, me in ((0, "tensor", z), (1, "fsdp_1", x), (2, "fsdp_0", y)):
        for k in (1, 2, 3):
            sum_copy(phase, axis, k, me).wait_send()
    share.wait()
    share_left.wait()
    share_norms.wait()
    for passing in passings:
        for o in range(4):
            for q in range(4):
                passing(o, q).wait()


def output_kernel(left, back, back_too, blended, blended_too, norms, momentum_new, update, basis_new, mom_v, up_v, base_v, sems):
    wide = COLS // CHUNKS
    dims = (((1,), (1,)), ((), ()))
    scale = math.sqrt(FEATURES * UNITS / RANK)
    me = lax.axis_index("replica")

    def copies(half, i):
        part = pl.ds(pl.multiple_of(i * wide, wide), wide)
        w = me if half == 0 else 1 - me
        return part, (
            pltpu.make_async_copy(base_v.at[half, part, :], basis_new.at[w, part, :], sems.at[0, half, i]),
            pltpu.make_async_copy(mom_v.at[half, :, part], momentum_new.at[w, :, part], sems.at[1, half, i]),
            pltpu.make_async_copy(up_v.at[half, :, part], update.at[w, :, part], sems.at[2, half, i]),
        )

    for half, (rows_ref, old) in enumerate(((back, blended), (back_too, blended_too))):
        inverse = 1.0 / (jnp.sqrt(jnp.sum(norms[half], axis=0, keepdims=True)) + 1e-06)
        basis = jnp.concatenate([left[half], (left[half].astype(F32) * inverse).astype(BF16)], axis=0)

        def chunk(i, carry, half=half, rows_ref=rows_ref, old=old, inverse=inverse, basis=basis):
            part, (base, mom, up) = copies(half, i)
            rows = rows_ref[part, :]
            normed = (rows.astype(F32) * inverse).astype(BF16)
            base_v[half, part, :] = normed
            base.start()
            product = lax.dot_general(basis, rows, dims, preferred_element_type=F32)
            value = old[:, part].astype(F32) - (1.0 - momentum_decay) * product[:ROWS]
            mom_v[half, :, part] = value.astype(BF16)
            mom.start()
            up_v[half, :, part] = (scale * product[ROWS:]).astype(BF16)
            up.start()
            return carry

        lax.fori_loop(0, CHUNKS, chunk, 0)
    for half in range(2):

        def finish(i, carry, half=half):
            for copy in copies(half, i)[1]:
                copy.wait()
            return carry

        lax.fori_loop(0, CHUNKS, finish, 0)


def shape(dims, dtype=BF16):
    return jax.ShapeDtypeStruct(dims, dtype)


VM = pl.BlockSpec(memory_space=pltpu.VMEM)
HBM = pl.BlockSpec(memory_space=pltpu.HBM)
DMA = pltpu.SemaphoreType.DMA


def shards(grads, momentum, basis):
    steps = COLS // STEP
    blended, blended_too, gathered, gathered_too, norms, left = pl.pallas_call(
        step_kernel,
        out_shape=(
            shape((ROWS, COLS)),
            shape((ROWS, COLS)),
            shape((4, 4, PIECE, RANK)),
            shape((4, 4, PIECE, RANK)),
            shape((2, 8, RANK), F32),
            shape((2, ROWS, RANK)),
        ),
        in_specs=[HBM] * 3,
        out_specs=(VM,) * 6,
        scratch_shapes=[
            pltpu.VMEM((ROWS, COLS), BF16),
            pltpu.VMEM((ROWS, COLS), BF16),
            pltpu.VMEM((ROWS, COLS), BF16),
            pltpu.VMEM((COLS, RANK), BF16),
            pltpu.VMEM((ROWS, RANK), F32),
            pltpu.VMEM((COLS, ROWS), BF16),
            pltpu.VMEM((3, SLICE, RANK), BF16),
            pltpu.VMEM((3, SLICE, RANK), BF16),
            pltpu.VMEM((4, 4, 4, SLICE, RANK), BF16),
            pltpu.VMEM((4, 4, PIECE, ROWS), BF16),
            pltpu.VMEM((RANK, RANK), F32),
            pltpu.VMEM((RANK, RANK), F32),
            pltpu.VMEM((BLOCK, 2 * BLOCK), F32),
            pltpu.VMEM((BLOCK, BLOCK), F32),
            pltpu.VMEM((PIECE, RANK), F32),
            pltpu.VMEM((3, 4, 8, RANK), F32),
            DMA((3, steps)),
            DMA((steps,)),
            DMA((steps,)),
            DMA((3,)),
            DMA((3,)),
            DMA((3, 2, 16)),
            DMA((3, 2, 16)),
            DMA((16,)),
            DMA((16,)),
            DMA((3,)),
            DMA((3,)),
            DMA((3, 3)),
            DMA((3, 3)),
            DMA((2, 32)),
            DMA((2, 32)),
        ],
        compiler_params=pltpu.CompilerParams(collective_id=0, has_side_effects=True, vmem_limit_bytes=42 << 20),
        name="step",
    )(grads, momentum, basis)
    return pl.pallas_call(
        output_kernel,
        out_shape=(shape((2, ROWS, COLS)), shape((2, ROWS, COLS)), shape((2, COLS, RANK))),
        in_specs=[VM] * 6,
        out_specs=(HBM,) * 3,
        scratch_shapes=[
            pltpu.VMEM((2, ROWS, COLS), BF16),
            pltpu.VMEM((2, ROWS, COLS), BF16),
            pltpu.VMEM((2, COLS, RANK), BF16),
            DMA((3, 2, CHUNKS)),
        ],
        compiler_params=pltpu.CompilerParams(vmem_limit_bytes=24 << 20),
        name="outputs",
    )(left, gathered.reshape(COLS, RANK), gathered_too.reshape(COLS, RANK), blended, blended_too, norms)


def solution(mesh):
    torus = Mesh(
        mesh.devices.reshape(mesh.shape["replica"], 4, 4, mesh.shape["tensor"]),
        ("replica", "fsdp_0", "fsdp_1", "tensor"),
    )
    return jax.shard_map(
        shards,
        mesh=torus,
        in_specs=(
            P("replica", None, FSDP, "tensor"),
            P(None, FSDP, "tensor"),
            P(None, "tensor", None),
        ),
        out_specs=(P(None, FSDP, "tensor"), P(None, FSDP, "tensor"), P(None, "tensor", None)),
        check_vma=False,
    )
```

```python
import functools
import math

import jax
import jax.numpy as jnp
from jax import lax
from jax.experimental import pallas as pl
from jax.experimental.pallas import tpu as pltpu
from jax.sharding import Mesh
from jax.sharding import PartitionSpec as P

FEATURES = 4096
UNITS = 14336
RANK = 512
FSDP = ("fsdp_0", "fsdp_1")
MESH = pl.DeviceIdType.MESH
BF16 = jnp.bfloat16
F32 = jnp.float32
ROWS = FEATURES // 16
COLS = UNITS // 4
PIECE = COLS // 16
SLICE = ROWS // 4
STEP = 512
PANEL = 16
BLOCK = 128
CHUNKS = 4

momentum_decay = 0.95


def coords():
    return tuple(lax.axis_index(a) for a in ("replica", "fsdp_0", "fsdp_1", "tensor"))


def shifted(i, k):
    return lax.rem(i + k, 4)


class Ring:
    def __init__(self, axis, at, send, recv):
        self.axis, self.at, self.send, self.recv = axis, at, send, recv

    def copy(self, k, arriving):
        me = lax.axis_index(self.axis)
        ref = self.at(shifted(me, 4 - k) if arriving else me)
        return pltpu.make_async_remote_copy(
            src_ref=ref,
            dst_ref=ref,
            send_sem=self.send.at[k],
            recv_sem=self.recv.at[k],
            device_id={self.axis: shifted(me, k)},
            device_id_type=MESH,
        )

    def start(self):
        for k in (2, 1, 3):
            self.copy(k, False).start()

    def end(self):
        for k in (1, 3, 2):
            self.copy(k, True).wait_recv()

    def drain(self):
        for k in (1, 2, 3):
            self.copy(k, False).wait_send()


def rows_of(start, size, half):
    if half is None:
        return pl.ds(start, size)
    return pl.ds(start + half * (size // 2), size // 2)


def projected_gather(full, y, x, z, send, recv):
    parts = ((0, 32, 0, 384), (32, 32, 0, 384), (0, 64, 384, 128))

    def cut(part, half):
        r0, nr, c0, nc = parts[part]
        return rows_of(r0, nr, half), pl.ds(c0, nc)

    every = slice(None)
    plans = (
        ("tensor", "fsdp_0", "fsdp_1", lambda i: (y, x, i), lambda o, q: (shifted(y, o), shifted(x, q), every)),
        ("fsdp_1", "tensor", "fsdp_0", lambda i: (y, i, z), lambda o, q: (shifted(y, q), every, shifted(z, o))),
        ("fsdp_0", "fsdp_1", "tensor", lambda i: (i, x, z), lambda o, q: (every, shifted(x, o), shifted(z, q))),
    )
    rings, spreads = [], []
    for part, (first, line, side, ring_at, spread_at) in enumerate(plans):
        def at_ring(i, part=part, where=ring_at):
            return full.at[(*where(i), *cut(part, None))]

        def at_spread(o, q, half, part=part, where=spread_at):
            return full.at[(*where(o, q), *cut(part, half))]

        rings.append(Ring(first, at_ring, send.at[part, 0], recv.at[part, 0]))
        spreads.append(Spread(at_spread, line, side, send.at[part, 1], recv.at[part, 1]))
    return rings, spreads


class Spread:
    def __init__(self, at, line_axis, side_axis, send, recv, hand=None):
        self.at, self.send, self.recv = at, send, recv
        self.line_axis, self.side_axis = line_axis, side_axis
        self.hand = hand or (lambda o, q: None)
        self.sent = []

    def copy(self, k, o, q, axis, way, half=None):
        ref = self.at(o, q, half)
        return pltpu.make_async_remote_copy(
            src_ref=ref,
            dst_ref=ref,
            send_sem=self.send.at[k],
            recv_sem=self.recv.at[k],
            device_id={axis: shifted(lax.axis_index(axis), way)},
            device_id_type=MESH,
        )

    def go(self, *args):
        copy = self.copy(*args)
        copy.start()
        self.sent.append(copy)

    def begin(self):
        self.go(0, 0, 0, self.line_axis, 1)
        self.go(1, 0, 0, self.line_axis, 3)
        self.sides(0)
        self.hand(0, 0)

    def sides(self, o):
        self.go(4 + o, o, 0, self.side_axis, 1)
        self.go(8 + o, o, 0, self.side_axis, 3)

    def line(self, o):
        if o == 3:
            self.copy(0, 3, 0, self.line_axis, 1).wait_recv()
            self.go(2, 3, 0, self.line_axis, 1, 0)
        elif o == 1:
            self.copy(1, 1, 0, self.line_axis, 3).wait_recv()
            self.go(3, 1, 0, self.line_axis, 3, 1)
        else:
            self.copy(2, 2, 0, self.line_axis, 1, 0).wait_recv()
            self.copy(3, 2, 0, self.line_axis, 3, 1).wait_recv()
        self.sides(o)
        self.hand(o, 0)

    def side(self, o):
        first, second = (3, 1) if o in (0, 3) else (1, 3)
        for q in (first, second):
            if q == 3:
                self.copy(4 + o, o, 3, self.side_axis, 1).wait_recv()
            else:
                self.copy(8 + o, o, 1, self.side_axis, 3).wait_recv()
            if q == first:
                self.go(12 + o, o, q, self.side_axis, 4 - q)
            self.hand(o, q)

    def last(self, o):
        self.copy(12 + o, o, 2, self.side_axis, 1 if o in (0, 3) else 3).wait_recv()
        self.hand(o, 2)

    def drain(self):
        for copy in self.sent:
            copy.wait_send()


SPREAD_STEPS = (("line", 3), ("line", 1), ("side", 0), ("line", 2), ("side", 3), ("side", 1), ("side", 2))


def together(spreads, job, *args):
    for spread in spreads:
        getattr(spread, job)(*args)


def halves(value):
    high = value.astype(BF16)
    return high, (value - high.astype(F32)).astype(BF16)


def contract_rows(a, b):
    ah, al = halves(a)
    bh, bl = halves(b)
    return lax.dot_general(
        jnp.concatenate([ah, ah, al], axis=0),
        jnp.concatenate([bh, bl, bh], axis=0),
        (((0,), (0,)), ((), ())),
        preferred_element_type=F32,
    )


def product(a, b):
    ah, al = halves(a)
    bh, bl = halves(b)
    return jnp.dot(
        jnp.concatenate([ah, ah, al], axis=1),
        jnp.concatenate([bh, bl, bh], axis=0),
        preferred_element_type=F32,
    )


def times_transpose(a, b):
    ah, al = halves(a)
    bh, bl = halves(b)
    return lax.dot_general(
        jnp.concatenate([ah, ah, al], axis=1),
        jnp.concatenate([bh, bl, bh], axis=1),
        (((1,), (1,)), ((), ())),
        preferred_element_type=F32,
    )


def eliminate(work, inverse):
    row = lax.broadcasted_iota(jnp.int32, (PANEL, BLOCK), 0)
    lane = lax.broadcasted_iota(jnp.int32, (BLOCK, BLOCK), 1)

    def panel(p, carry):
        left, right = work[0:PANEL, 0:BLOCK], work[0:PANEL, BLOCK:]
        columns = [jnp.broadcast_to(left[:, k : k + 1], (PANEL, BLOCK)) for k in range(PANEL)]
        inverses = jnp.ones((PANEL, BLOCK), F32)
        for j in range(PANEL):
            inv = 1.0 / columns[j][j : j + 1, :]
            times = jnp.where(row > j, columns[j] * inv, 0.0)
            for k in range(j + 1, PANEL):
                columns[k] = columns[k] - times * columns[k][j : j + 1, :]
            left = left - times * left[j : j + 1, :]
            right = right - times * right[j : j + 1, :]
            inverses = jnp.where(row == j, inv, inverses)
        scale = jnp.sqrt(inverses)
        left, right = left * scale, right * scale
        inverse[pl.ds(pl.multiple_of(p * PANEL, PANEL), PANEL), :] = right
        change = contract_rows(left, jnp.concatenate([left, right], axis=1))
        rest = work[:, 0:BLOCK] - change[:, 0:BLOCK]
        rest = jnp.where(lane < BLOCK - PANEL, pltpu.roll(rest, BLOCK - PANEL, 1), 0.0)
        work[0 : BLOCK - PANEL, 0:BLOCK] = rest[PANEL:, :]
        extra = work[:, BLOCK:] - change[:, BLOCK:]
        work[0 : BLOCK - PANEL, BLOCK:] = extra[PANEL:, :]
        work[BLOCK - PANEL :, :] = jnp.zeros((PANEL, 2 * BLOCK), F32)
        return carry

    lax.fori_loop(0, BLOCK // PANEL, panel, 0)


def factor_inverse(gram, low, work, inverse):
    low[...] = jnp.zeros_like(low)
    count = RANK // BLOCK
    square = (BLOCK, BLOCK)
    eye = jnp.where(
        lax.broadcasted_iota(jnp.int32, square, 0) == lax.broadcasted_iota(jnp.int32, square, 1), 1.0, 0.0
    )
    for k in range(count):
        here, after = slice(k * BLOCK, (k + 1) * BLOCK), slice((k + 1) * BLOCK, RANK)
        work[:, 0:BLOCK] = gram[here, here]
        work[:, BLOCK:] = eye
        eliminate(work, inverse)
        block = inverse[...]
        if k:
            low[here, 0 : k * BLOCK] = product(block, low[here, 0 : k * BLOCK])
        low[here, here] = block
        if k < count - 1:
            upper = product(block, gram[here, after])
            gram[after, after] = gram[after, after] - contract_rows(upper, upper)
            done = slice(0, (k + 1) * BLOCK)
            low[after, done] = low[after, done] - contract_rows(upper, low[here, done])


def meet(y, x, z, other):
    barrier = pltpu.get_barrier_semaphore()
    peers = [{"replica": other}] + [{"tensor": shifted(z, k)} for k in (1, 2, 3)]
    peers += [{"fsdp_0": shifted(y, k // 4), "fsdp_1": shifted(x, k % 4)} for k in range(1, 16)]
    for peer in peers:
        pl.semaphore_signal(barrier, inc=1, device_id=peer, device_id_type=MESH)
    pl.semaphore_wait(barrier, len(peers))


def step_kernel(
    grads, momentum, basis, blended, blended_too, gathered, gathered_too, norms, left,
    m_v, g_v, gp_v, b_v, acc, flipped, out_z, in_z, full, turned, gram, low, work, inverse, total, sums,
    load, gs, gr, zs, zr, ags, agr, ts, tr, bs, br, s_n, r_n, s_p, r_p,
):
    r, y, x, z = coords()
    other = 1 - r
    steps = COLS // STEP

    def grad_copy(c, cols):
        return pltpu.make_async_remote_copy(
            src_ref=grads.at[0, other, :, cols],
            dst_ref=gp_v.at[:, cols],
            send_sem=gs.at[c],
            recv_sem=gr.at[c],
            device_id={"replica": other},
            device_id_type=MESH,
        )

    def loads(c, cols):
        return (
            pltpu.make_async_copy(grads.at[0, r, :, cols], g_v.at[:, cols], load.at[0, c]),
            pltpu.make_async_copy(momentum.at[r, :, cols], m_v.at[:, cols], load.at[1, c]),
            pltpu.make_async_copy(basis.at[r, cols, :], b_v.at[cols, :], load.at[2, c]),
        )

    for c in range(steps):
        for copy in loads(c, pl.ds(c * STEP, STEP)):
            copy.start()
    meet(y, x, z, other)
    for c in range(steps):
        grad_copy(c, pl.ds(c * STEP, STEP)).start()
    acc[...] = jnp.zeros_like(acc)

    def blend(c, carry):
        cols = pl.ds(pl.multiple_of(c * STEP, STEP), STEP)
        for copy in loads(c, cols):
            copy.wait()
        grad_copy(c, cols).wait()
        both = g_v[:, cols].astype(F32) + gp_v[:, cols].astype(F32)
        value = (m_v[:, cols].astype(F32) + both).astype(BF16)
        blended[:, cols] = value
        acc[...] += jnp.dot(value, b_v[cols, :], preferred_element_type=F32)
        return carry

    lax.fori_loop(0, steps, blend, 0)

    def z_copy(k):
        return pltpu.make_async_remote_copy(
            src_ref=out_z.at[k - 1],
            dst_ref=in_z.at[k - 1],
            send_sem=zs.at[k - 1],
            recv_sem=zr.at[k - 1],
            device_id={"tensor": shifted(z, k)},
            device_id_type=MESH,
        )

    for k in (2, 1, 3):
        rows = pl.ds(pl.multiple_of(shifted(z, k) * SLICE, SLICE), SLICE)
        out_z[k - 1] = acc[rows, :].astype(BF16)
        z_copy(k).start()

    def flip(c, carry):
        cols = pl.ds(pl.multiple_of(c * STEP, STEP), STEP)
        flipped[cols, :] = blended[:, cols].T
        return carry

    lax.fori_loop(0, steps, flip, 0)
    def turn_copy(k):
        ty, tx = shifted(y, k // 4), shifted(x, k % 4)
        start = pl.multiple_of((ty * 4 + tx) * PIECE, PIECE)
        return pltpu.make_async_remote_copy(
            src_ref=flipped.at[pl.ds(start, PIECE), :],
            dst_ref=turned.at[y, x],
            send_sem=ts.at[k],
            recv_sem=tr.at[k],
            device_id={"fsdp_0": ty, "fsdp_1": tx},
            device_id_type=MESH,
        )

    piece = acc[pl.ds(pl.multiple_of(z * SLICE, SLICE), SLICE), :]
    for k in (1, 3, 2):
        z_copy(k).wait()
        piece = piece + in_z[k - 1].astype(F32)
    full[y, x, z] = piece.astype(BF16)

    rings, wide = projected_gather(full, y, x, z, ags, agr)
    together(rings, "start")
    together(rings, "end")
    together(wide, "begin")
    for job, o in SPREAD_STEPS:
        together(wide, job, o)

    def turn_arrival(k):
        sy, sx = shifted(y, 4 - k // 4), shifted(x, 4 - k % 4)
        return pltpu.make_async_remote_copy(
            src_ref=turned.at[sy, sx],
            dst_ref=turned.at[sy, sx],
            send_sem=ts.at[k],
            recv_sem=tr.at[k],
            device_id={"fsdp_0": sy, "fsdp_1": sx},
            device_id_type=MESH,
        )

    for k in range(1, 16):
        turn_copy(k).start()

    def to_partner(src, dst, send, recv):
        return pltpu.make_async_remote_copy(
            src_ref=src,
            dst_ref=dst,
            send_sem=send,
            recv_sem=recv,
            device_id={"replica": other},
            device_id_type=MESH,
        )

    share = to_partner(blended, blended_too, bs.at[0], br.at[0])
    share.start()
    turned[y, x] = flipped[pl.ds(pl.multiple_of((y * 4 + x) * PIECE, PIECE), PIECE), :]
    for o in (0, 3, 1, 2):
        together(wide, "last", o)

    gram[...] = jnp.zeros_like(gram)

    def add_gram(b, carry):
        rows = full[b].reshape(4 * ROWS, RANK)
        gram[...] += lax.dot_general(rows, rows, (((0,), (0,)), ((), ())), preferred_element_type=F32)
        return carry

    lax.fori_loop(0, 4, add_gram, 0)
    factor_inverse(gram, low, work, inverse)
    high = low[...].astype(BF16)
    total[...] = jnp.zeros_like(total)
    dims = (((1,), (1,)), ((), ()))

    def left_rows(rows):
        return lax.dot_general(rows, high, dims, preferred_element_type=F32).astype(BF16)

    for k in range(1, 16):
        turn_copy(k).wait_send()
        turn_arrival(k).wait_recv()

    def add_back(b, carry):
        rows = full[b].reshape(4 * ROWS, RANK)
        columns = jnp.concatenate([turned[b, bx] for bx in range(4)], axis=1)
        total[...] += jnp.dot(columns, rows, preferred_element_type=F32)
        return carry

    lax.fori_loop(0, 4, add_back, 0)
    value = times_transpose(total[...], low[...])
    gathered[y, x] = value.astype(BF16)

    def sum_copy(phase, axis, k, me):
        return pltpu.make_async_remote_copy(
            src_ref=sums.at[phase, me],
            dst_ref=sums.at[phase, me],
            send_sem=s_n.at[phase, k - 1],
            recv_sem=r_n.at[phase, k - 1],
            device_id={axis: shifted(me, k)},
            device_id_type=MESH,
        )

    def sum_arrival(phase, axis, k, me):
        source = shifted(me, 4 - k)
        return pltpu.make_async_remote_copy(
            src_ref=sums.at[phase, source],
            dst_ref=sums.at[phase, source],
            send_sem=s_n.at[phase, k - 1],
            recv_sem=r_n.at[phase, k - 1],
            device_id={axis: source},
            device_id_type=MESH,
        )

    def send_sums(phase, axis, me, block):
        sums[phase, me] = block
        for k in (2, 1, 3):
            sum_copy(phase, axis, k, me).start()

    def take_sums(phase, axis, me):
        for k in (1, 3, 2):
            sum_arrival(phase, axis, k, me).wait_recv()
        return (sums[phase, 0] + sums[phase, 1]) + (sums[phase, 2] + sums[phase, 3])

    def spread_of(part):
        cols = pl.ds(part * (RANK // 2), RANK // 2)
        axes = ("fsdp_0", "fsdp_1") if part == 0 else ("fsdp_1", "fsdp_0")

        def place(o, q):
            return (shifted(y, o), shifted(x, q)) if part == 0 else (shifted(y, q), shifted(x, o))

        def at(o, q, half):
            return gathered.at[(*place(o, q), rows_of(0, PIECE, half), cols)]

        def passing(o, q):
            where = (*place(o, q), slice(None), cols)
            k = 16 + 4 * o + q
            return to_partner(gathered.at[where], gathered_too.at[where], s_p.at[part, k], r_p.at[part, k])

        def hand(o, q):
            passing(o, q).start()

        return Spread(at, *axes, s_p.at[part], r_p.at[part], hand), passing

    spreads, passings = zip(*(spread_of(part) for part in (0, 1)))
    together(spreads, "begin")
    send_sums(0, "tensor", z, jnp.sum((value * value).reshape(PIECE // 8, 8, RANK), axis=0))
    left[0] = left_rows(full[y, x].reshape(ROWS, RANK))
    share_left = to_partner(left.at[0], left.at[1], bs.at[1], br.at[1])
    share_left.start()
    for at_step, (job, o) in enumerate(SPREAD_STEPS):
        together(spreads, job, o)
        if at_step == 1:
            send_sums(1, "fsdp_1", x, take_sums(0, "tensor", z))
        elif at_step == 3:
            send_sums(2, "fsdp_0", y, take_sums(1, "fsdp_1", x))
        elif at_step == 5:
            norms[0] = take_sums(2, "fsdp_0", y)
            share_norms = to_partner(norms.at[0], norms.at[1], bs.at[2], br.at[2])
            share_norms.start()
    for o in (0, 3, 1, 2):
        together(spreads, "last", o)
    together(spreads, "drain")
    together(rings, "drain")
    together(wide, "drain")
    for phase, axis, me in ((0, "tensor", z), (1, "fsdp_1", x), (2, "fsdp_0", y)):
        for k in (1, 2, 3):
            sum_copy(phase, axis, k, me).wait_send()
    share.wait()
    share_left.wait()
    share_norms.wait()
    for passing in passings:
        for o in range(4):
            for q in range(4):
                passing(o, q).wait()


def output_kernel(left, back, back_too, blended, blended_too, norms, momentum_new, update, basis_new, mom_v, up_v, base_v, sems):
    wide = COLS // CHUNKS
    dims = (((1,), (1,)), ((), ()))
    scale = math.sqrt(FEATURES * UNITS / RANK)
    me = lax.axis_index("replica")

    def copies(half, i):
        part = pl.ds(pl.multiple_of(i * wide, wide), wide)
        w = me if half == 0 else 1 - me
        return part, (
            pltpu.make_async_copy(base_v.at[half, part, :], basis_new.at[w, part, :], sems.at[0, half, i]),
            pltpu.make_async_copy(mom_v.at[half, :, part], momentum_new.at[w, :, part], sems.at[1, half, i]),
            pltpu.make_async_copy(up_v.at[half, :, part], update.at[w, :, part], sems.at[2, half, i]),
        )

    for half, (rows_ref, old) in enumerate(((back, blended), (back_too, blended_too))):
        inverse = 1.0 / (jnp.sqrt(jnp.sum(norms[half], axis=0, keepdims=True)) + 1e-06)
        basis = jnp.concatenate([left[half], (left[half].astype(F32) * inverse).astype(BF16)], axis=0)

        def chunk(i, carry, half=half, rows_ref=rows_ref, old=old, inverse=inverse, basis=basis):
            part, (base, mom, up) = copies(half, i)
            rows = rows_ref[part, :]
            normed = (rows.astype(F32) * inverse).astype(BF16)
            base_v[half, part, :] = normed
            base.start()
            product = lax.dot_general(basis, rows, dims, preferred_element_type=F32)
            value = old[:, part].astype(F32) - (1.0 - momentum_decay) * product[:ROWS]
            mom_v[half, :, part] = value.astype(BF16)
            mom.start()
            up_v[half, :, part] = (scale * product[ROWS:]).astype(BF16)
            up.start()
            return carry

        lax.fori_loop(0, CHUNKS, chunk, 0)
    for half in range(2):

        def finish(i, carry, half=half):
            for copy in copies(half, i)[1]:
                copy.wait()
            return carry

        lax.fori_loop(0, CHUNKS, finish, 0)


def shape(dims, dtype=BF16):
    return jax.ShapeDtypeStruct(dims, dtype)


VM = pl.BlockSpec(memory_space=pltpu.VMEM)
HBM = pl.BlockSpec(memory_space=pltpu.HBM)
DMA = pltpu.SemaphoreType.DMA


def shards(grads, momentum, basis):
    steps = COLS // STEP
    blended, blended_too, gathered, gathered_too, norms, left = pl.pallas_call(
        step_kernel,
        out_shape=(
            shape((ROWS, COLS)),
            shape((ROWS, COLS)),
            shape((4, 4, PIECE, RANK)),
            shape((4, 4, PIECE, RANK)),
            shape((2, 8, RANK), F32),
            shape((2, ROWS, RANK)),
        ),
        in_specs=[HBM] * 3,
        out_specs=(VM,) * 6,
        scratch_shapes=[
            pltpu.VMEM((ROWS, COLS), BF16),
            pltpu.VMEM((ROWS, COLS), BF16),
            pltpu.VMEM((ROWS, COLS), BF16),
            pltpu.VMEM((COLS, RANK), BF16),
            pltpu.VMEM((ROWS, RANK), F32),
            pltpu.VMEM((COLS, ROWS), BF16),
            pltpu.VMEM((3, SLICE, RANK), BF16),
            pltpu.VMEM((3, SLICE, RANK), BF16),
            pltpu.VMEM((4, 4, 4, SLICE, RANK), BF16),
            pltpu.VMEM((4, 4, PIECE, ROWS), BF16),
            pltpu.VMEM((RANK, RANK), F32),
            pltpu.VMEM((RANK, RANK), F32),
            pltpu.VMEM((BLOCK, 2 * BLOCK), F32),
            pltpu.VMEM((BLOCK, BLOCK), F32),
            pltpu.VMEM((PIECE, RANK), F32),
            pltpu.VMEM((3, 4, 8, RANK), F32),
            DMA((3, steps)),
            DMA((steps,)),
            DMA((steps,)),
            DMA((3,)),
            DMA((3,)),
            DMA((3, 2, 16)),
            DMA((3, 2, 16)),
            DMA((16,)),
            DMA((16,)),
            DMA((3,)),
            DMA((3,)),
            DMA((3, 3)),
            DMA((3, 3)),
            DMA((2, 32)),
            DMA((2, 32)),
        ],
        compiler_params=pltpu.CompilerParams(collective_id=0, has_side_effects=True, vmem_limit_bytes=42 << 20),
        name="step",
    )(grads, momentum, basis)
    return pl.pallas_call(
        output_kernel,
        out_shape=(shape((2, ROWS, COLS)), shape((2, ROWS, COLS)), shape((2, COLS, RANK))),
        in_specs=[VM] * 6,
        out_specs=(HBM,) * 3,
        scratch_shapes=[
            pltpu.VMEM((2, ROWS, COLS), BF16),
            pltpu.VMEM((2, ROWS, COLS), BF16),
            pltpu.VMEM((2, COLS, RANK), BF16),
            DMA((3, 2, CHUNKS)),
        ],
        compiler_params=pltpu.CompilerParams(vmem_limit_bytes=24 << 20),
        name="outputs",
    )(left, gathered.reshape(COLS, RANK), gathered_too.reshape(COLS, RANK), blended, blended_too, norms)


def solution(mesh):
    torus = Mesh(
        mesh.devices.reshape(mesh.shape["replica"], 4, 4, mesh.shape["tensor"]),
        ("replica", "fsdp_0", "fsdp_1", "tensor"),
    )
    return jax.shard_map(
        shards,
        mesh=torus,
        in_specs=(
            P("replica", None, FSDP, "tensor"),
            P(None, FSDP, "tensor"),
            P(None, "tensor", None),
        ),
        out_specs=(P(None, FSDP, "tensor"), P(None, FSDP, "tensor"), P(None, "tensor", None)),
        check_vma=False,
    )
```

```python
import functools
import math

import jax
import jax.numpy as jnp
from jax import lax
from jax.experimental import pallas as pl
from jax.experimental.pallas import tpu as pltpu
from jax.sharding import Mesh
from jax.sharding import PartitionSpec as P

FEATURES = 4096
UNITS = 14336
RANK = 512
FSDP = ("fsdp_0", "fsdp_1")
MESH = pl.DeviceIdType.MESH
BF16 = jnp.bfloat16
F32 = jnp.float32
ROWS = FEATURES // 16
COLS = UNITS // 4
PIECE = COLS // 16
SLICE = ROWS // 4
STEP = 512
PANEL = 16
BLOCK = 128
CHUNKS = 2

momentum_decay = 0.95


def coords():
    return tuple(lax.axis_index(a) for a in ("replica", "fsdp_0", "fsdp_1", "tensor"))


def shifted(i, k):
    return lax.rem(i + k, 4)


class Ring:
    def __init__(self, axis, at, send, recv):
        self.axis, self.at, self.send, self.recv = axis, at, send, recv

    def copy(self, k, arriving):
        me = lax.axis_index(self.axis)
        ref = self.at(shifted(me, 4 - k) if arriving else me)
        return pltpu.make_async_remote_copy(
            src_ref=ref,
            dst_ref=ref,
            send_sem=self.send.at[k],
            recv_sem=self.recv.at[k],
            device_id={self.axis: shifted(me, k)},
            device_id_type=MESH,
        )

    def start(self):
        for k in (2, 1, 3):
            self.copy(k, False).start()

    def end(self):
        for k in (1, 3, 2):
            self.copy(k, True).wait_recv()

    def drain(self):
        for k in (1, 2, 3):
            self.copy(k, False).wait_send()


def rows_of(start, size, half):
    if half is None:
        return pl.ds(start, size)
    return pl.ds(start + half * (size // 2), size // 2)


def projected_gather(full, y, x, z, send, recv):
    parts = ((0, 32, 0, 384), (32, 32, 0, 384), (0, 64, 384, 128))

    def cut(part, half):
        r0, nr, c0, nc = parts[part]
        return rows_of(r0, nr, half), pl.ds(c0, nc)

    every = slice(None)
    plans = (
        ("tensor", "fsdp_0", "fsdp_1", lambda i: (y, x, i), lambda o, q: (shifted(y, o), shifted(x, q), every)),
        ("fsdp_1", "tensor", "fsdp_0", lambda i: (y, i, z), lambda o, q: (shifted(y, q), every, shifted(z, o))),
        ("fsdp_0", "fsdp_1", "tensor", lambda i: (i, x, z), lambda o, q: (every, shifted(x, o), shifted(z, q))),
    )
    rings, spreads = [], []
    for part, (first, line, side, ring_at, spread_at) in enumerate(plans):
        def at_ring(i, part=part, where=ring_at):
            return full.at[(*where(i), *cut(part, None))]

        def at_spread(o, q, half, part=part, where=spread_at):
            return full.at[(*where(o, q), *cut(part, half))]

        rings.append(Ring(first, at_ring, send.at[part, 0], recv.at[part, 0]))
        spreads.append(Spread(at_spread, line, side, send.at[part, 1], recv.at[part, 1]))
    return rings, spreads


class Spread:
    def __init__(self, at, line_axis, side_axis, send, recv, hand=None):
        self.at, self.send, self.recv = at, send, recv
        self.line_axis, self.side_axis = line_axis, side_axis
        self.hand = hand or (lambda o, q: None)
        self.sent = []

    def copy(self, k, o, q, axis, way, half=None):
        ref = self.at(o, q, half)
        return pltpu.make_async_remote_copy(
            src_ref=ref,
            dst_ref=ref,
            send_sem=self.send.at[k],
            recv_sem=self.recv.at[k],
            device_id={axis: shifted(lax.axis_index(axis), way)},
            device_id_type=MESH,
        )

    def go(self, *args):
        copy = self.copy(*args)
        copy.start()
        self.sent.append(copy)

    def begin(self):
        self.go(0, 0, 0, self.line_axis, 1)
        self.go(1, 0, 0, self.line_axis, 3)
        self.sides(0)
        self.hand(0, 0)

    def sides(self, o):
        self.go(4 + o, o, 0, self.side_axis, 1)
        self.go(8 + o, o, 0, self.side_axis, 3)

    def line(self, o):
        if o == 3:
            self.copy(0, 3, 0, self.line_axis, 1).wait_recv()
            self.go(2, 3, 0, self.line_axis, 1, 0)
        elif o == 1:
            self.copy(1, 1, 0, self.line_axis, 3).wait_recv()
            self.go(3, 1, 0, self.line_axis, 3, 1)
        else:
            self.copy(2, 2, 0, self.line_axis, 1, 0).wait_recv()
            self.copy(3, 2, 0, self.line_axis, 3, 1).wait_recv()
        self.sides(o)
        self.hand(o, 0)

    def side(self, o):
        first, second = (3, 1) if o in (0, 3) else (1, 3)
        for q in (first, second):
            if q == 3:
                self.copy(4 + o, o, 3, self.side_axis, 1).wait_recv()
            else:
                self.copy(8 + o, o, 1, self.side_axis, 3).wait_recv()
            if q == first:
                self.go(12 + o, o, q, self.side_axis, 4 - q)
            self.hand(o, q)

    def last(self, o):
        self.copy(12 + o, o, 2, self.side_axis, 1 if o in (0, 3) else 3).wait_recv()
        self.hand(o, 2)

    def drain(self):
        for copy in self.sent:
            copy.wait_send()


SPREAD_STEPS = (("line", 3), ("line", 1), ("side", 0), ("line", 2), ("side", 3), ("side", 1), ("side", 2))


def together(spreads, job, *args):
    for spread in spreads:
        getattr(spread, job)(*args)


def halves(value):
    high = value.astype(BF16)
    return high, (value - high.astype(F32)).astype(BF16)


def contract_rows(a, b):
    ah, al = halves(a)
    bh, bl = halves(b)
    return lax.dot_general(
        jnp.concatenate([ah, ah, al], axis=0),
        jnp.concatenate([bh, bl, bh], axis=0),
        (((0,), (0,)), ((), ())),
        preferred_element_type=F32,
    )


def product(a, b):
    ah, al = halves(a)
    bh, bl = halves(b)
    return jnp.dot(
        jnp.concatenate([ah, ah, al], axis=1),
        jnp.concatenate([bh, bl, bh], axis=0),
        preferred_element_type=F32,
    )


def times_transpose(a, b):
    ah, al = halves(a)
    bh, bl = halves(b)
    return lax.dot_general(
        jnp.concatenate([ah, ah, al], axis=1),
        jnp.concatenate([bh, bl, bh], axis=1),
        (((1,), (1,)), ((), ())),
        preferred_element_type=F32,
    )


def eliminate(work, inverse):
    row = lax.broadcasted_iota(jnp.int32, (PANEL, BLOCK), 0)
    lane = lax.broadcasted_iota(jnp.int32, (BLOCK, BLOCK), 1)

    def panel(p, carry):
        left, right = work[0:PANEL, 0:BLOCK], work[0:PANEL, BLOCK:]
        columns = [jnp.broadcast_to(left[:, k : k + 1], (PANEL, BLOCK)) for k in range(PANEL)]
        inverses = jnp.ones((PANEL, BLOCK), F32)
        for j in range(PANEL):
            inv = 1.0 / columns[j][j : j + 1, :]
            times = jnp.where(row > j, columns[j] * inv, 0.0)
            for k in range(j + 1, PANEL):
                columns[k] = columns[k] - times * columns[k][j : j + 1, :]
            left = left - times * left[j : j + 1, :]
            right = right - times * right[j : j + 1, :]
            inverses = jnp.where(row == j, inv, inverses)
        scale = jnp.sqrt(inverses)
        left, right = left * scale, right * scale
        inverse[pl.ds(pl.multiple_of(p * PANEL, PANEL), PANEL), :] = right
        change = contract_rows(left, jnp.concatenate([left, right], axis=1))
        rest = work[:, 0:BLOCK] - change[:, 0:BLOCK]
        rest = jnp.where(lane < BLOCK - PANEL, pltpu.roll(rest, BLOCK - PANEL, 1), 0.0)
        work[0 : BLOCK - PANEL, 0:BLOCK] = rest[PANEL:, :]
        extra = work[:, BLOCK:] - change[:, BLOCK:]
        work[0 : BLOCK - PANEL, BLOCK:] = extra[PANEL:, :]
        work[BLOCK - PANEL :, :] = jnp.zeros((PANEL, 2 * BLOCK), F32)
        return carry

    lax.fori_loop(0, BLOCK // PANEL, panel, 0)


def factor_inverse(gram, low, work, inverse):
    low[...] = jnp.zeros_like(low)
    count = RANK // BLOCK
    square = (BLOCK, BLOCK)
    eye = jnp.where(
        lax.broadcasted_iota(jnp.int32, square, 0) == lax.broadcasted_iota(jnp.int32, square, 1), 1.0, 0.0
    )
    for k in range(count):
        here, after = slice(k * BLOCK, (k + 1) * BLOCK), slice((k + 1) * BLOCK, RANK)
        work[:, 0:BLOCK] = gram[here, here]
        work[:, BLOCK:] = eye
        eliminate(work, inverse)
        block = inverse[...]
        if k:
            low[here, 0 : k * BLOCK] = product(block, low[here, 0 : k * BLOCK])
        low[here, here] = block
        if k < count - 1:
            upper = product(block, gram[here, after])
            gram[after, after] = gram[after, after] - contract_rows(upper, upper)
            done = slice(0, (k + 1) * BLOCK)
            low[after, done] = low[after, done] - contract_rows(upper, low[here, done])


def meet(y, x, z, other):
    barrier = pltpu.get_barrier_semaphore()
    peers = [{"replica": other}] + [{"tensor": shifted(z, k)} for k in (1, 2, 3)]
    peers += [{"fsdp_0": shifted(y, k // 4), "fsdp_1": shifted(x, k % 4)} for k in range(1, 16)]
    for peer in peers:
        pl.semaphore_signal(barrier, inc=1, device_id=peer, device_id_type=MESH)
    pl.semaphore_wait(barrier, len(peers))


def step_kernel(
    grads, momentum, basis, blended, blended_too, gathered, gathered_too, norms, left,
    m_v, g_v, gp_v, b_v, acc, flipped, out_z, in_z, full, turned, gram, low, work, inverse, total, sums,
    load, gs, gr, zs, zr, ags, agr, ts, tr, bs, br, s_n, r_n, s_p, r_p,
):
    r, y, x, z = coords()
    other = 1 - r
    steps = COLS // STEP

    def grad_copy(c, cols):
        return pltpu.make_async_remote_copy(
            src_ref=grads.at[0, other, :, cols],
            dst_ref=gp_v.at[:, cols],
            send_sem=gs.at[c],
            recv_sem=gr.at[c],
            device_id={"replica": other},
            device_id_type=MESH,
        )

    def loads(c, cols):
        return (
            pltpu.make_async_copy(grads.at[0, r, :, cols], g_v.at[:, cols], load.at[0, c]),
            pltpu.make_async_copy(momentum.at[r, :, cols], m_v.at[:, cols], load.at[1, c]),
            pltpu.make_async_copy(basis.at[r, cols, :], b_v.at[cols, :], load.at[2, c]),
        )

    for c in range(steps):
        for copy in loads(c, pl.ds(c * STEP, STEP)):
            copy.start()
    meet(y, x, z, other)
    for c in range(steps):
        grad_copy(c, pl.ds(c * STEP, STEP)).start()
    acc[...] = jnp.zeros_like(acc)

    def blend(c, carry):
        cols = pl.ds(pl.multiple_of(c * STEP, STEP), STEP)
        for copy in loads(c, cols):
            copy.wait()
        grad_copy(c, cols).wait()
        both = g_v[:, cols].astype(F32) + gp_v[:, cols].astype(F32)
        value = (m_v[:, cols].astype(F32) + both).astype(BF16)
        blended[:, cols] = value
        acc[...] += jnp.dot(value, b_v[cols, :], preferred_element_type=F32)
        return carry

    lax.fori_loop(0, steps, blend, 0)

    def z_copy(k):
        return pltpu.make_async_remote_copy(
            src_ref=out_z.at[k - 1],
            dst_ref=in_z.at[k - 1],
            send_sem=zs.at[k - 1],
            recv_sem=zr.at[k - 1],
            device_id={"tensor": shifted(z, k)},
            device_id_type=MESH,
        )

    for k in (2, 1, 3):
        rows = pl.ds(pl.multiple_of(shifted(z, k) * SLICE, SLICE), SLICE)
        out_z[k - 1] = acc[rows, :].astype(BF16)
        z_copy(k).start()

    def flip(c, carry):
        cols = pl.ds(pl.multiple_of(c * STEP, STEP), STEP)
        flipped[cols, :] = blended[:, cols].T
        return carry

    lax.fori_loop(0, steps, flip, 0)
    def turn_copy(k):
        ty, tx = shifted(y, k // 4), shifted(x, k % 4)
        start = pl.multiple_of((ty * 4 + tx) * PIECE, PIECE)
        return pltpu.make_async_remote_copy(
            src_ref=flipped.at[pl.ds(start, PIECE), :],
            dst_ref=turned.at[y, x],
            send_sem=ts.at[k],
            recv_sem=tr.at[k],
            device_id={"fsdp_0": ty, "fsdp_1": tx},
            device_id_type=MESH,
        )

    piece = acc[pl.ds(pl.multiple_of(z * SLICE, SLICE), SLICE), :]
    for k in (1, 3, 2):
        z_copy(k).wait()
        piece = piece + in_z[k - 1].astype(F32)
    full[y, x, z] = piece.astype(BF16)

    rings, wide = projected_gather(full, y, x, z, ags, agr)
    together(rings, "start")
    together(rings, "end")
    together(wide, "begin")
    for job, o in SPREAD_STEPS:
        together(wide, job, o)

    def turn_arrival(k):
        sy, sx = shifted(y, 4 - k // 4), shifted(x, 4 - k % 4)
        return pltpu.make_async_remote_copy(
            src_ref=turned.at[sy, sx],
            dst_ref=turned.at[sy, sx],
            send_sem=ts.at[k],
            recv_sem=tr.at[k],
            device_id={"fsdp_0": sy, "fsdp_1": sx},
            device_id_type=MESH,
        )

    for k in range(1, 16):
        turn_copy(k).start()

    def to_partner(src, dst, send, recv):
        return pltpu.make_async_remote_copy(
            src_ref=src,
            dst_ref=dst,
            send_sem=send,
            recv_sem=recv,
            device_id={"replica": other},
            device_id_type=MESH,
        )

    share = to_partner(blended, blended_too, bs.at[0], br.at[0])
    share.start()
    turned[y, x] = flipped[pl.ds(pl.multiple_of((y * 4 + x) * PIECE, PIECE), PIECE), :]
    for o in (0, 3, 1, 2):
        together(wide, "last", o)

    gram[...] = jnp.zeros_like(gram)

    def add_gram(b, carry):
        rows = full[b].reshape(4 * ROWS, RANK)
        gram[...] += lax.dot_general(rows, rows, (((0,), (0,)), ((), ())), preferred_element_type=F32)
        return carry

    lax.fori_loop(0, 4, add_gram, 0)
    factor_inverse(gram, low, work, inverse)
    high = low[...].astype(BF16)
    total[...] = jnp.zeros_like(total)
    dims = (((1,), (1,)), ((), ()))

    def left_rows(rows):
        return lax.dot_general(rows, high, dims, preferred_element_type=F32).astype(BF16)

    for k in range(1, 16):
        turn_copy(k).wait_send()
        turn_arrival(k).wait_recv()

    def add_back(b, carry):
        rows = full[b].reshape(4 * ROWS, RANK)
        columns = jnp.concatenate([turned[b, bx] for bx in range(4)], axis=1)
        total[...] += jnp.dot(columns, rows, preferred_element_type=F32)
        return carry

    lax.fori_loop(0, 4, add_back, 0)
    value = times_transpose(total[...], low[...])
    gathered[y, x] = value.astype(BF16)

    def sum_copy(phase, axis, k, me):
        return pltpu.make_async_remote_copy(
            src_ref=sums.at[phase, me],
            dst_ref=sums.at[phase, me],
            send_sem=s_n.at[phase, k - 1],
            recv_sem=r_n.at[phase, k - 1],
            device_id={axis: shifted(me, k)},
            device_id_type=MESH,
        )

    def sum_arrival(phase, axis, k, me):
        source = shifted(me, 4 - k)
        return pltpu.make_async_remote_copy(
            src_ref=sums.at[phase, source],
            dst_ref=sums.at[phase, source],
            send_sem=s_n.at[phase, k - 1],
            recv_sem=r_n.at[phase, k - 1],
            device_id={axis: source},
            device_id_type=MESH,
        )

    def send_sums(phase, axis, me, block):
        sums[phase, me] = block
        for k in (2, 1, 3):
            sum_copy(phase, axis, k, me).start()

    def take_sums(phase, axis, me):
        for k in (1, 3, 2):
            sum_arrival(phase, axis, k, me).wait_recv()
        return (sums[phase, 0] + sums[phase, 1]) + (sums[phase, 2] + sums[phase, 3])

    def spread_of(part):
        cols = pl.ds(part * (RANK // 2), RANK // 2)
        axes = ("fsdp_0", "fsdp_1") if part == 0 else ("fsdp_1", "fsdp_0")

        def place(o, q):
            return (shifted(y, o), shifted(x, q)) if part == 0 else (shifted(y, q), shifted(x, o))

        def at(o, q, half):
            return gathered.at[(*place(o, q), rows_of(0, PIECE, half), cols)]

        def passing(o, q):
            where = (*place(o, q), slice(None), cols)
            k = 16 + 4 * o + q
            return to_partner(gathered.at[where], gathered_too.at[where], s_p.at[part, k], r_p.at[part, k])

        def hand(o, q):
            passing(o, q).start()

        return Spread(at, *axes, s_p.at[part], r_p.at[part], hand), passing

    spreads, passings = zip(*(spread_of(part) for part in (0, 1)))
    together(spreads, "begin")
    send_sums(0, "tensor", z, jnp.sum((value * value).reshape(PIECE // 8, 8, RANK), axis=0))
    left[0] = left_rows(full[y, x].reshape(ROWS, RANK))
    share_left = to_partner(left.at[0], left.at[1], bs.at[1], br.at[1])
    share_left.start()
    for at_step, (job, o) in enumerate(SPREAD_STEPS):
        together(spreads, job, o)
        if at_step == 1:
            send_sums(1, "fsdp_1", x, take_sums(0, "tensor", z))
        elif at_step == 3:
            send_sums(2, "fsdp_0", y, take_sums(1, "fsdp_1", x))
        elif at_step == 5:
            norms[0] = take_sums(2, "fsdp_0", y)
            share_norms = to_partner(norms.at[0], norms.at[1], bs.at[2], br.at[2])
            share_norms.start()
    for o in (0, 3, 1, 2):
        together(spreads, "last", o)
    together(spreads, "drain")
    together(rings, "drain")
    together(wide, "drain")
    for phase, axis, me in ((0, "tensor", z), (1, "fsdp_1", x), (2, "fsdp_0", y)):
        for k in (1, 2, 3):
            sum_copy(phase, axis, k, me).wait_send()
    share.wait()
    share_left.wait()
    share_norms.wait()
    for passing in passings:
        for o in range(4):
            for q in range(4):
                passing(o, q).wait()


def output_kernel(left, back, back_too, blended, blended_too, norms, momentum_new, update, basis_new, mom_v, up_v, base_v, sems):
    wide = COLS // CHUNKS
    dims = (((1,), (1,)), ((), ()))
    scale = math.sqrt(FEATURES * UNITS / RANK)
    me = lax.axis_index("replica")

    def copies(half, i):
        part = pl.ds(pl.multiple_of(i * wide, wide), wide)
        w = me if half == 0 else 1 - me
        return part, (
            pltpu.make_async_copy(base_v.at[half, part, :], basis_new.at[w, part, :], sems.at[0, half, i]),
            pltpu.make_async_copy(mom_v.at[half, :, part], momentum_new.at[w, :, part], sems.at[1, half, i]),
            pltpu.make_async_copy(up_v.at[half, :, part], update.at[w, :, part], sems.at[2, half, i]),
        )

    for half, (rows_ref, old) in enumerate(((back, blended), (back_too, blended_too))):
        inverse = 1.0 / (jnp.sqrt(jnp.sum(norms[half], axis=0, keepdims=True)) + 1e-06)
        basis = jnp.concatenate([left[half], (left[half].astype(F32) * inverse).astype(BF16)], axis=0)

        def chunk(i, carry, half=half, rows_ref=rows_ref, old=old, inverse=inverse, basis=basis):
            part, (base, mom, up) = copies(half, i)
            rows = rows_ref[part, :]
            normed = (rows.astype(F32) * inverse).astype(BF16)
            base_v[half, part, :] = normed
            base.start()
            product = lax.dot_general(basis, rows, dims, preferred_element_type=F32)
            value = old[:, part].astype(F32) - (1.0 - momentum_decay) * product[:ROWS]
            mom_v[half, :, part] = value.astype(BF16)
            mom.start()
            up_v[half, :, part] = (scale * product[ROWS:]).astype(BF16)
            up.start()
            return carry

        lax.fori_loop(0, CHUNKS, chunk, 0)
    for half in range(2):

        def finish(i, carry, half=half):
            for copy in copies(half, i)[1]:
                copy.wait()
            return carry

        lax.fori_loop(0, CHUNKS, finish, 0)


def shape(dims, dtype=BF16):
    return jax.ShapeDtypeStruct(dims, dtype)


VM = pl.BlockSpec(memory_space=pltpu.VMEM)
HBM = pl.BlockSpec(memory_space=pltpu.HBM)
DMA = pltpu.SemaphoreType.DMA


def shards(grads, momentum, basis):
    steps = COLS // STEP
    blended, blended_too, gathered, gathered_too, norms, left = pl.pallas_call(
        step_kernel,
        out_shape=(
            shape((ROWS, COLS)),
            shape((ROWS, COLS)),
            shape((4, 4, PIECE, RANK)),
            shape((4, 4, PIECE, RANK)),
            shape((2, 8, RANK), F32),
            shape((2, ROWS, RANK)),
        ),
        in_specs=[HBM] * 3,
        out_specs=(VM,) * 6,
        scratch_shapes=[
            pltpu.VMEM((ROWS, COLS), BF16),
            pltpu.VMEM((ROWS, COLS), BF16),
            pltpu.VMEM((ROWS, COLS), BF16),
            pltpu.VMEM((COLS, RANK), BF16),
            pltpu.VMEM((ROWS, RANK), F32),
            pltpu.VMEM((COLS, ROWS), BF16),
            pltpu.VMEM((3, SLICE, RANK), BF16),
            pltpu.VMEM((3, SLICE, RANK), BF16),
            pltpu.VMEM((4, 4, 4, SLICE, RANK), BF16),
            pltpu.VMEM((4, 4, PIECE, ROWS), BF16),
            pltpu.VMEM((RANK, RANK), F32),
            pltpu.VMEM((RANK, RANK), F32),
            pltpu.VMEM((BLOCK, 2 * BLOCK), F32),
            pltpu.VMEM((BLOCK, BLOCK), F32),
            pltpu.VMEM((PIECE, RANK), F32),
            pltpu.VMEM((3, 4, 8, RANK), F32),
            DMA((3, steps)),
            DMA((steps,)),
            DMA((steps,)),
            DMA((3,)),
            DMA((3,)),
            DMA((3, 2, 16)),
            DMA((3, 2, 16)),
            DMA((16,)),
            DMA((16,)),
            DMA((3,)),
            DMA((3,)),
            DMA((3, 3)),
            DMA((3, 3)),
            DMA((2, 32)),
            DMA((2, 32)),
        ],
        compiler_params=pltpu.CompilerParams(collective_id=0, has_side_effects=True, vmem_limit_bytes=42 << 20),
        name="step",
    )(grads, momentum, basis)
    return pl.pallas_call(
        output_kernel,
        out_shape=(shape((2, ROWS, COLS)), shape((2, ROWS, COLS)), shape((2, COLS, RANK))),
        in_specs=[VM] * 6,
        out_specs=(HBM,) * 3,
        scratch_shapes=[
            pltpu.VMEM((2, ROWS, COLS), BF16),
            pltpu.VMEM((2, ROWS, COLS), BF16),
            pltpu.VMEM((2, COLS, RANK), BF16),
            DMA((3, 2, CHUNKS)),
        ],
        compiler_params=pltpu.CompilerParams(vmem_limit_bytes=24 << 20),
        name="outputs",
    )(left, gathered.reshape(COLS, RANK), gathered_too.reshape(COLS, RANK), blended, blended_too, norms)


def solution(mesh):
    torus = Mesh(
        mesh.devices.reshape(mesh.shape["replica"], 4, 4, mesh.shape["tensor"]),
        ("replica", "fsdp_0", "fsdp_1", "tensor"),
    )
    return jax.shard_map(
        shards,
        mesh=torus,
        in_specs=(
            P("replica", None, FSDP, "tensor"),
            P(None, FSDP, "tensor"),
            P(None, "tensor", None),
        ),
        out_specs=(P(None, FSDP, "tensor"), P(None, FSDP, "tensor"), P(None, "tensor", None)),
        check_vma=False,
    )
```
